32 devices in a mesh: cls: 4 (over y, x), str: 8 (over z, core).
Axes of the slice: x: 2, y: 2, z: 4, core: 2. Of those that a mesh axis runs over, the one named last changes fastest.
Arguments:
- first_factor_tiles: float32 [8, 1024, 2, 4, 1024], P(None, ('cls', 'str')), may hold values from -6 to 6
- b_blocks: float32 [8, 1024, 2, 4, 512], P(None, ('cls', 'str')), may hold values from -0.0625 to 0.0625
Outputs:
- c_blocks: float32 [8, 1024, 2, 4, 512], P(None, ('cls', 'str'))
The draws below stay inside these ranges and needn't reach their ends.
All inputs are finite; a program needn't handle non-finite values.
Results may differ from the reference program's by a relative error of at most 0.0003.
Values sent between devices are 32-bit elements; how exact they have to be, the bound alone decides.
A program may use at most 128 MiB of HBM per device.

```python
import jax
import jax.numpy as jnp
import numpy as np
from jax import lax

N = 8192
Q = 1024
QC = 512


def block_levels(key, extent, split, low, largest):
    level = 1.0
    for position, parts in split:
        draws = jax.random.uniform(jax.random.fold_in(jax.random.fold_in(key, 6), position), (parts,), jnp.float32, low / len(split), largest / len(split))
        level = level * jnp.repeat(jnp.exp(draws), extent[position] // parts).reshape((-1,) + (1,) * (len(extent) - 1 - position))
    return level


def scatter_about(key, dims, width, bound, shards=(), kind=jnp.bfloat16):
    drawn = width * jax.random.normal(key, dims, jnp.float32)
    if shards:
        drawn = drawn * block_levels(key, dims, shards, -0.22, 0.18)
    return jnp.clip(drawn, -bound, bound).astype(kind)


def setup_inputs(seed: int = 0) -> dict:
    key_of = jax.random.split(jax.random.key(seed), 3)
    return {
        "first_factor_tiles": scatter_about(key_of[0], (8, Q, 2, 4, Q), 1.0, 6.0, ((1, 32),), jnp.float32),
        "b_blocks": scatter_about(key_of[1], (8, Q, 2, 4, QC), N ** -0.5, 0.0625, ((1, 32),), jnp.float32),
    }


def strassen_weight_lists():
    left_base = np.array([[1, 0, 0, 0], [0, 1, 0, 0], [1, 1, -1, -1], [0, 0, 0, 1], [0, 0, 1, 1], [-1, 0, 1, 1], [1, 0, -1, 0]], np.float32)
    right_base_matrix = np.array([[1, 0, 0, 0], [0, 0, 1, 0], [0, 0, 0, 1], [1, -1, -1, 1], [-1, 1, 0, 0], [1, -1, 0, 1], [0, -1, 0, 1]], np.float32)
    product_grid_start = np.array([[1, 1, 0, 0, 0, 0, 0], [1, 0, 1, 0, 1, 1, 0], [1, 0, 0, -1, 0, 1, 1], [1, 0, 0, 0, 1, 1, 1]], np.float32)
    left_split = left_base.reshape(7, 2, 2)
    right_split = right_base_matrix.reshape(7, 2, 2)
    outer_split = product_grid_start.reshape(2, 2, 7)
    left_table = (left_split[:, None, :, None, :, None] * left_split[None, :, None, :, None, :]).reshape(49, 4, 4)
    right_table = (right_split[:, None, :, None, :, None] * right_split[None, :, None, :, None, :]).reshape(49, 4, 4)
    outer_table = (outer_split[:, None, :, None, :, None] * outer_split[None, :, None, :, None, :]).reshape(4, 4, 49)
    return left_table, right_table, outer_table


def reference(first_factor_tiles, b_blocks):
    first_factor_host_grid, second_factor_host_grid, product_host_grid = strassen_weight_lists()
    left_table = jnp.asarray(first_factor_host_grid).astype(first_factor_tiles.dtype)
    right_table = jnp.asarray(second_factor_host_grid).astype(first_factor_tiles.dtype)
    outer_table = jnp.asarray(product_host_grid).astype(first_factor_tiles.dtype)
    product_ids = np.arange(8)
    inner_halves = product_ids // 4
    row_half_split = (product_ids // 2) % 2
    col_halves = product_ids % 2
    a_six = first_factor_tiles.reshape(2, 4, Q, 2, 4, Q)
    b_six = b_blocks.reshape(2, 4, Q, 2, 4, QC)
    left_stack = a_six[row_half_split, :, :, inner_halves]
    right_stack = b_six[inner_halves, :, :, col_halves]
    highest = lax.Precision.HIGHEST

    def leaf_product(pair):
        x_quad, y_quad = pair
        left_leaves = jnp.einsum('mac,aqcr->mqr', left_table, x_quad, precision=highest)
        right_leaves = jnp.einsum('mac,aqcr->mqr', right_table, y_quad, precision=highest)
        leaf_out = jnp.einsum('mqk,mkr->mqr', left_leaves, right_leaves, precision=highest)
        return jnp.einsum('acm,mqr->aqcr', outer_table, leaf_out, precision=highest)

    partials = lax.map(leaf_product, (left_stack, right_stack))
    partials = partials.reshape(2, 2, 2, 4, Q, 4, QC)
    summed = partials[0] + partials[1]
    summed = jnp.transpose(summed, (0, 2, 3, 1, 4, 5))
    return summed.reshape(8, Q, 2, 4, QC)
```

```python
import functools

import jax
import jax.numpy as jnp
from jax import lax
from jax.experimental import pallas as pl
from jax.experimental.pallas import tpu as pltpu
from jax.sharding import PartitionSpec as P

MESH = pl.DeviceIdType.MESH
LAG = 3
EARLY = 2
AHEAD = 6
LEAD = 2
LANE = 128
SUBLANE = 8


def flip(index, mask, count):
    out, bit = index, 1
    while bit < count:
        have, want = (index // bit) % 2, (mask // bit) % 2
        out = out + want * (1 - 2 * have) * bit
        bit *= 2
    return out


def kernel(
    classes, subs, a_ref, b_ref, o_ref, aland, ball,
    ahi, alo, astage, bstage, bhi, blo, cpart, rland,
    a_send, a_recv, own_send, fwd_send, line_recv, peer_send, peer_recv,
    c_send, c_recv, a_load, b_load, o_sem,
):
    chunks, groups, piece, width = b_ref.shape
    rows = a_ref.shape[1]
    depth = subs * piece
    spots = subs // 2
    c, s = lax.axis_index("cls"), lax.axis_index("str")
    spot, core = s // 2, s % 2
    mate = (c, s + 1 - 2 * core)
    beside = ((c, s - 2), (c, s + 2))
    has = (spot > 0, spot < spots - 1)

    barrier = pltpu.get_barrier_semaphore()
    for d in range(1, classes):
        pl.semaphore_signal(barrier, inc=1, device_id=(flip(c, d, classes), s), device_id_type=MESH)
    pl.semaphore_signal(barrier, inc=1, device_id=mate, device_id_type=MESH)
    for side in range(2):
        @pl.when(has[side])
        def _():
            pl.semaphore_signal(barrier, inc=1, device_id=beside[side], device_id_type=MESH)
    lower, higher = (spot + spots - 1) // spots, (2 * spots - 2 - spot) // spots
    pl.semaphore_wait(barrier, classes + lower + higher)

    def remote(src, dst, send, recv, to):
        return pltpu.make_async_remote_copy(
            src_ref=src, dst_ref=dst, send_sem=send, recv_sem=recv,
            device_id=to, device_id_type=MESH,
        )

    def slot(j, owner):
        return ball.at[j, :, pl.ds(pl.multiple_of(owner * piece, piece), piece), :]

    def own_line(j, side):
        return remote(b_ref.at[j], slot(j, s), own_send.at[side, j], line_recv.at[side, j, 0], beside[side])

    def own_mate(j):
        return remote(b_ref.at[j], slot(j, s), peer_send.at[j, spot], peer_recv.at[j, spot], mate)

    def origin(side, dist):
        return spot + dist if side == 0 else spot - dist

    def there(side, dist):
        return spot + dist < spots if side == 0 else spot >= dist

    def arrival(j, side, dist):
        at = slot(j, 2 * origin(side, dist) + core)
        return remote(at, at, own_send.at[side, j], line_recv.at[side, j, dist - 1], beside[1 - side])

    def onward(j, side, dist):
        at = slot(j, 2 * origin(side, dist) + core)
        return remote(at, at, fwd_send.at[side, j, dist - 1], line_recv.at[side, j, dist], beside[side])

    def across(j, side, dist):
        begin = origin(side, dist)
        at = slot(j, 2 * begin + core)
        return remote(at, at, peer_send.at[j, begin], peer_recv.at[j, begin], mate)

    def forward(j, dist):
        for side in range(2):
            @pl.when(there(side, dist))
            def _():
                arrival(j, side, dist).wait_recv()

                @pl.when(has[side])
                def _():
                    onward(j, side, dist).start()

                across(j, side, dist).start()

    def a_copy(d):
        peer = flip(c, d, classes)
        return remote(
            a_ref.at[:, :, pl.ds(pl.multiple_of(peer * depth, depth), depth)],
            aland.at[:, pl.ds(pl.multiple_of(c * rows, rows), rows), :],
            a_send.at[d], a_recv.at[d], (peer, s),
        )

    for d in range(1, classes):
        a_copy(d).start()

    def begin(j, _):
        for side in range(2):
            @pl.when(has[side])
            def _():
                own_line(j, side).start()
        own_mate(j).start()
        return 0

    lax.fori_loop(0, chunks, begin, 0)

    for j in range(min(EARLY, chunks)):
        forward(j, 1)
    for d in range(1, classes):
        a_copy(d).wait_recv()

    def load_a(g, held):
        for e in range(classes):
            to = astage.at[held, pl.ds(e * rows, rows), :]

            @pl.when(c == e)
            def _():
                pltpu.make_async_copy(
                    a_ref.at[g, :, pl.ds(pl.multiple_of(c * depth, depth), depth)], to, a_load.at[held]
                ).start()

            @pl.when(c != e)
            def _():
                pltpu.make_async_copy(aland.at[g, pl.ds(e * rows, rows), :], to, a_load.at[held]).start()

    load_a(0, 0)
    for g in range(groups):
        held = g % 2
        if g + 1 < groups:
            load_a(g + 1, 1 - held)
        pltpu.make_async_copy(aland.at[g], astage.at[held], a_load.at[held]).wait()

        def split(m, _, held=held, g=g):
            at = pl.ds(pl.multiple_of(m * rows, rows), rows)
            value = astage[held, at, :]
            high = value.astype(jnp.bfloat16)
            ahi[at, g * depth:(g + 1) * depth] = high
            alo[at, g * depth:(g + 1) * depth] = (value - high.astype(jnp.float32)).astype(jnp.bfloat16)
            return 0

        lax.fori_loop(0, classes, split, 0)

    def c_copy(j, d):
        peer = flip(c, d, classes)
        return remote(
            cpart.at[j, pl.ds(pl.multiple_of(peer * rows, rows), rows), :],
            rland.at[j, d - 1], c_send.at[j, d], c_recv.at[j, d], (peer, s),
        )

    mine = pl.ds(pl.multiple_of(c * rows, rows), rows)

    def out_copy(j):
        return pltpu.make_async_copy(cpart.at[j, mine, :], o_ref.at[j], o_sem.at[j])

    def reduce(j):
        for d in range(1, classes):
            c_copy(j, d).wait_recv()
        total = cpart[j, mine, :]
        for d in range(1, classes):
            total = total + rland[j, d - 1]
        cpart[j, mine, :] = total
        out_copy(j).start()

    def step(j, _):
        if spots > 1:
            @pl.when(j + EARLY < chunks)
            def _():
                forward(j + EARLY, 1)
        for dist in range(2, spots):
            forward(j, dist)

        for owner in range(subs):
            to = bstage.at[:, pl.ds(owner * piece, piece), :]

            @pl.when(s == owner)
            def _():
                pltpu.make_async_copy(b_ref.at[j], to, b_load.at[0]).start()

            @pl.when(s != owner)
            def _():
                @pl.when(core != owner % 2)
                def _():
                    remote(to_slot(j, owner), to_slot(j, owner), peer_send.at[j, owner // 2],
                           peer_recv.at[j, owner // 2], mate).wait_recv()

                pltpu.make_async_copy(to_slot(j, owner), to, b_load.at[0]).start()

        pltpu.make_async_copy(ball.at[j], bstage, b_load.at[0]).wait()

        def split(g, _):
            value = bstage[g]
            high = value.astype(jnp.bfloat16)
            at = pl.ds(pl.multiple_of(g * depth, depth), depth)
            bhi[at, :] = high
            blo[at, :] = (value - high.astype(jnp.float32)).astype(jnp.bfloat16)
            return 0

        lax.fori_loop(0, groups, split, 0)

        def part(i, _):
            d = (i + 1) % classes
            at = pl.ds(pl.multiple_of(flip(c, d, classes) * rows, rows), rows)
            dot = functools.partial(jnp.dot, preferred_element_type=jnp.float32)
            cpart[j, at, :] = (
                dot(ahi[at, :], bhi[...]) + dot(ahi[at, :], blo[...]) + dot(alo[at, :], bhi[...])
            )

            @pl.when(d != 0)
            def _():
                c_copy(j, d).start()

            return 0

        lax.fori_loop(0, classes, part, 0)

        @pl.when(j >= LAG)
        def _():
            reduce(j - LAG)

        return 0

    def to_slot(j, owner):
        return ball.at[j, :, pl.ds(owner * piece, piece), :]

    lax.fori_loop(0, chunks, step, 0)
    for j in range(max(chunks - LAG, 0), chunks):
        reduce(j)

    def finish(j, _):
        out_copy(j).wait()
        own_mate(j).wait_send()
        for d in range(1, classes):
            c_copy(j, d).wait_send()
        for side in range(2):
            @pl.when(has[side])
            def _():
                own_line(j, side).wait_send()
            for dist in range(1, spots):
                @pl.when(there(side, dist))
                def _():
                    @pl.when(has[side])
                    def _():
                        onward(j, side, dist).wait_send()
                    across(j, side, dist).wait_send()
        return 0

    lax.fori_loop(0, chunks, finish, 0)
    for d in range(1, classes):
        a_copy(d).wait_send()


def local(classes, subs, first_factor_tiles, b_blocks):
    blocks, q, halves, cols, order = first_factor_tiles.shape
    inner, width = halves * cols, b_blocks.shape[4]
    rows = blocks * q
    left = first_factor_tiles.reshape(rows, inner, order)
    right = jnp.transpose(b_blocks.reshape(inner, q, inner, width), (2, 0, 1, 3))
    if q % 8 == 0:
        left = jnp.transpose(left, (1, 0, 2))
    else:
        left = left.reshape(rows, inner, classes * subs, q)
        left = jnp.transpose(left, (0, 2, 1, 3)).reshape(1, rows, inner * order)
        right = right.reshape(inner, 1, inner * q, width)
    chunks, groups, piece, _ = right.shape
    depth = subs * piece
    dma = pltpu.SemaphoreType.DMA
    f32, bf16 = jnp.float32, jnp.bfloat16
    spots = subs // 2
    out, _, _ = pl.pallas_call(
        functools.partial(kernel, classes, subs),
        out_shape=(
            jax.ShapeDtypeStruct((chunks, rows, width), f32),
            jax.ShapeDtypeStruct((groups, classes * rows, depth), f32),
            jax.ShapeDtypeStruct((chunks, groups, depth, width), f32),
        ),
        in_specs=[pl.BlockSpec(memory_space=pl.ANY)] * 2,
        out_specs=(pl.BlockSpec(memory_space=pl.ANY),) * 3,
        scratch_shapes=[
            pltpu.VMEM((classes * rows, groups * depth), bf16),
            pltpu.VMEM((classes * rows, groups * depth), bf16),
            pltpu.VMEM((2, classes * rows, depth), f32),
            pltpu.VMEM((groups, depth, width), f32),
            pltpu.VMEM((groups * depth, width), bf16),
            pltpu.VMEM((groups * depth, width), bf16),
            pltpu.VMEM((chunks, classes * rows, width), f32),
            pltpu.VMEM((chunks, classes - 1, rows, width), f32),
            dma((classes,)),
            dma((classes,)),
            dma((2, chunks)),
            dma((2, chunks, spots)),
            dma((2, chunks, spots)),
            dma((chunks, spots)),
            dma((chunks, spots)),
            dma((chunks, classes)),
            dma((chunks, classes)),
            dma((2,)),
            dma((1,)),
            dma((chunks,)),
        ],
        compiler_params=pltpu.CompilerParams(
            collective_id=0, has_side_effects=True, vmem_limit_bytes=60 * 1024 * 1024
        ),
    )(left, right)
    out = jnp.transpose(out, (1, 0, 2))
    return out.reshape(b_blocks.shape)


def stream(
    classes, subs, a_ref, b_ref, o_ref, aland, ball,
    flat, bown, astage, ahi, alo, bstage, bhi, blo, cpart, rland,
    a_send, a_recv, own_send, fwd_send, line_recv, peer_send, peer_recv, keep_sem,
    c_send, c_recv, a_load, b_load, o_sem,
):
    lead, _, unit, lane = a_ref.shape
    rows, ncol, _ = b_ref.shape
    chunks, blocks, depth, width = ball.shape
    bands = depth // lane
    piece = depth // subs
    per = width // lane
    levels = classes.bit_length() - 1
    spots = subs // 2
    c, s = lax.axis_index("cls"), lax.axis_index("str")
    spot, core = s // 2, s % 2
    mate = (c, s + 1 - 2 * core)
    beside = ((c, s - 2), (c, s + 2))
    has = (spot > 0, spot < spots - 1)
    inner = (spot > 0) & (spot < spots - 1)
    outer = (spot == 0) | (spot == spots - 1)
    near = spot // (spots // bands)

    barrier = pltpu.get_barrier_semaphore()
    for d in range(1, classes):
        pl.semaphore_signal(barrier, inc=1, device_id=(flip(c, d, classes), s), device_id_type=MESH)
    pl.semaphore_signal(barrier, inc=1, device_id=mate, device_id_type=MESH)
    for side in range(2):
        @pl.when(has[side])
        def _():
            pl.semaphore_signal(barrier, inc=1, device_id=beside[side], device_id_type=MESH)
    b_in = pltpu.make_async_copy(b_ref, flat, b_load.at[0])
    b_in.start()
    lower, higher = (spot + spots - 1) // spots, (2 * spots - 2 - spot) // spots
    pl.semaphore_wait(barrier, classes + lower + higher)

    def remote(src, dst, send, recv, to):
        return pltpu.make_async_remote_copy(
            src_ref=src, dst_ref=dst, send_sem=send, recv_sem=recv,
            device_id=to, device_id_type=MESH,
        )

    def a_copy(d):
        peer = flip(c, d, classes)
        return remote(a_ref.at[:, peer], aland.at[d - 1], a_send.at[d], a_recv.at[d], (peer, s))

    for d in range(1, classes):
        a_copy(d).start()

    def slot(j, owner):
        return ball.at[j, :, pl.ds(pl.multiple_of(owner * piece, piece), piece), :]

    def own_line(j, side):
        return remote(bown.at[j], slot(j, s), own_send.at[side, j], line_recv.at[side, j, 0], beside[side])

    def own_mate(j):
        return remote(bown.at[j], slot(j, s), peer_send.at[j, spot], peer_recv.at[j, spot], mate)

    def own_keep(j):
        return pltpu.make_async_copy(bown.at[j], slot(j, s), keep_sem.at[j])

    def origin(side, dist):
        return spot + dist if side == 0 else spot - dist

    def there(side, dist):
        return spot + dist < spots if side == 0 else spot >= dist

    def arrival(j, side, dist):
        at = slot(j, 2 * origin(side, dist) + core)
        return remote(at, at, own_send.at[side, j], line_recv.at[side, j, dist - 1], beside[1 - side])

    def onward(j, side, dist):
        at = slot(j, 2 * origin(side, dist) + core)
        return remote(at, at, fwd_send.at[side, j, dist - 1], line_recv.at[side, j, dist], beside[side])

    def across(j, side, dist):
        begin = origin(side, dist)
        at = slot(j, 2 * begin + core)
        return remote(at, at, peer_send.at[j, begin], peer_recv.at[j, begin], mate)

    def forward(j, dist):
        for side in range(2):
            @pl.when(there(side, dist))
            def _():
                arrival(j, side, dist).wait_recv()

                @pl.when(has[side])
                def _():
                    onward(j, side, dist).start()

                across(j, side, dist).start()

    def own_out(j):
        for side in range(2):
            @pl.when(has[side])
            def _():
                own_line(j, side).start()

    b_in.wait()
    rows_of = flat.reshape(rows * ncol, lane)

    def lay(j):
        for p in range(per):
            value = rows_of[pl.ds(j * per + p, rows, stride=ncol), :]
            bown[j, :, :, p * lane:(p + 1) * lane] = value.reshape(blocks, piece, lane)

    for j in range(min(LEAD, chunks)):
        lay(j)
    for j in range(min(LEAD, chunks)):
        own_out(j)

    def lay_more(j, _):
        lay(j)
        return 0

    lax.fori_loop(min(LEAD, chunks), chunks, lay_more, 0)

    def begin(j, _):
        own_mate(j).start()
        own_keep(j).start()

        @pl.when(outer & (j >= LEAD))
        def _():
            own_out(j)

        return 0

    lax.fori_loop(0, chunks, begin, 0)

    def take_a(d):
        held = astage.at[d % 2]
        if d == 0:
            return pltpu.make_async_copy(a_ref.at[:, c], held, a_load.at[0])
        return pltpu.make_async_copy(aland.at[d - 1], held, a_load.at[d % 2])

    def split_a(d):
        lines = astage.at[d % 2].reshape(lead * unit, lane)
        stride = lead * unit // rows
        cols = unit // bands

        def one(k, _):
            h, band, col = k // unit, (k % unit) // cols, k % cols
            value = lines[pl.ds(k, rows, stride=stride), :]
            high = value.astype(jnp.bfloat16)
            at = pl.ds(pl.multiple_of((h * cols + col) * lane, lane), lane)
            ahi[band, d * rows:(d + 1) * rows, at] = high
            alo[band, d * rows:(d + 1) * rows, at] = (value - high.astype(jnp.float32)).astype(jnp.bfloat16)
            return 0

        lax.fori_loop(0, stride, one, 0)

    take_a(0).start()
    take_a(0).wait()
    split_a(0)

    @pl.when(inner)
    def _():
        def early(j, _):
            for dist in range(1, spots):
                forward(j, dist)

            @pl.when(j + LEAD < chunks)
            def _():
                own_out(j + LEAD)

            return 0

        lax.fori_loop(0, min(AHEAD, chunks), early, 0)

    for d in range(1, classes):
        a_copy(d).wait_recv()
        take_a(d).start()
        if d > 1:
            take_a(d - 1).wait()
            split_a(d - 1)
    take_a(classes - 1).wait()
    split_a(classes - 1)

    def order(p):
        return [(p + i) % levels for i in range(levels)]

    def place(p, d):
        at = 0
        for bit in order(p):
            at = 2 * at + (d // (1 << bit)) % 2
        return at

    def c_copy(j, p, level):
        count = classes >> (level + 1)
        peer = flip(c, 1 << order(p)[level], classes)
        return remote(
            cpart.at[j, p, pl.ds(count, count)],
            rland.at[j, p, pl.ds(classes - 2 * count, count)],
            c_send.at[j, p, level], c_recv.at[j, p, level], (peer, s),
        )

    share = ncol // o_sem.shape[0]

    def out_copy(g):
        at = pl.ds(pl.multiple_of(g * share, share), share)
        return pltpu.make_async_copy(flat.at[:, at, :], o_ref.at[:, at, :], o_sem.at[g])

    def reduce(j, level):
        count = classes >> (level + 1)
        for p in range(per):
            c_copy(j, p, level).wait_recv()
            if level + 1 < levels:
                cpart[j, p, 0:count] = (
                    cpart[j, p, 0:count] + rland[j, p, classes - 2 * count:classes - count]
                )
                c_copy(j, p, level + 1).start()
            else:
                rows_of[pl.ds(j * per + p, rows, stride=ncol), :] = (
                    cpart[j, p, 0] + rland[j, p, classes - 2]
                )
        if level + 1 == levels:
            @pl.when((j + 1) % (share // per) == 0)
            def _():
                out_copy((j + 1) // (share // per) - 1).start()

    def hold(j, band):
        for owner in range(subs):
            @pl.when(owner // (subs // bands) == band)
            def _():
                @pl.when(s == owner)
                def _():
                    own_keep(j).wait()

                @pl.when(core != owner % 2)
                def _():
                    at = slot(j, owner)
                    remote(at, at, peer_send.at[j, owner // 2], peer_recv.at[j, owner // 2], mate).wait_recv()

        take = pltpu.make_async_copy(
            ball.at[j, :, pl.ds(pl.multiple_of(band * lane, lane), lane), :], bstage, b_load.at[0]
        )
        take.start()
        take.wait()

        def split(g, _):
            value = bstage[g]
            high = value.astype(jnp.bfloat16)
            at = pl.ds(pl.multiple_of(g * lane, lane), lane)
            bhi[at, :] = high
            blo[at, :] = (value - high.astype(jnp.float32)).astype(jnp.bfloat16)
            return 0

        lax.fori_loop(0, blocks, split, 0)

    def multiply(j, band, first):
        dot = functools.partial(jnp.dot, preferred_element_type=jnp.float32)

        def part(d, _):
            at = pl.ds(pl.multiple_of(d * rows, rows), rows)
            high, low = ahi[band, at, :], alo[band, at, :]
            total = dot(high, bhi[...]) + dot(high, blo[...]) + dot(low, bhi[...])
            for p in range(per):
                value = total[:, p * lane:(p + 1) * lane]
                to = place(p, d)
                cpart[j, p, to] = value if first else cpart[j, p, to] + value
            return 0

        lax.fori_loop(0, classes, part, 0)

    def step(j, _):
        @pl.when(inner & (j + AHEAD < chunks))
        def _():
            for dist in range(1, spots):
                forward(j + AHEAD, dist)

            @pl.when(j + AHEAD + LEAD < chunks)
            def _():
                own_out(j + AHEAD + LEAD)

        @pl.when(outer)
        def _():
            forward(j, 1)

        hold(j, near)
        multiply(j, near, True)

        @pl.when(j >= 1)
        def _():
            reduce(j - 1, 0)

        if levels > 1:
            @pl.when(j >= 2)
            def _():
                for level in range(1, levels):
                    reduce(j - 2, level)

        @pl.when(outer)
        def _():
            for dist in range(2, spots):
                forward(j, dist)

        for k in range(1, bands):
            band = (near + k) % bands
            hold(j, band)
            multiply(j, band, False)
        for p in range(per):
            c_copy(j, p, 0).start()
        return 0

    lax.fori_loop(0, chunks, step, 0)
    for level in range(1, levels):
        reduce(chunks - 2, level)
    for level in range(levels):
        reduce(chunks - 1, level)
    for g in range(o_sem.shape[0]):
        out_copy(g).wait()

    def finish(j, _):
        own_mate(j).wait_send()
        for p in range(per):
            for level in range(levels):
                c_copy(j, p, level).wait_send()
        for side in range(2):
            @pl.when(has[side])
            def _():
                own_line(j, side).wait_send()
            for dist in range(1, spots):
                @pl.when(there(side, dist))
                def _():
                    @pl.when(has[side])
                    def _():
                        onward(j, side, dist).wait_send()
                    across(j, side, dist).wait_send()
        return 0

    lax.fori_loop(0, chunks, finish, 0)
    for d in range(1, classes):
        a_copy(d).wait_send()


def streamed(classes, subs, first_factor_tiles, b_blocks):
    blocks, q, halves, cols, order = first_factor_tiles.shape
    wide = b_blocks.shape[4]
    lane, sub = LANE, SUBLANE
    rows, bands, ncol = blocks * q, order // (LANE * classes), halves * cols * wide // LANE
    left = first_factor_tiles.reshape(rows, halves, cols, classes * bands, lane)
    left = jnp.transpose(left, (0, 1, 3, 2, 4)).reshape(rows * halves, classes, bands * cols, lane)
    right = b_blocks.reshape(rows, halves, cols, wide // lane, lane)
    right = jnp.transpose(right, (0, 1, 3, 2, 4)).reshape(rows, ncol, lane)
    lead, unit = rows * halves, bands * cols
    per = 2
    chunks, width, depth = ncol // per, per * lane, bands * lane
    dma = pltpu.SemaphoreType.DMA
    f32, bf16 = jnp.float32, jnp.bfloat16
    spots, levels = subs // 2, classes.bit_length() - 1
    out, _, _ = pl.pallas_call(
        functools.partial(stream, classes, subs),
        out_shape=(
            jax.ShapeDtypeStruct((rows, ncol, lane), f32),
            jax.ShapeDtypeStruct((classes - 1, lead, unit, lane), f32),
            jax.ShapeDtypeStruct((chunks, blocks, depth, width), f32),
        ),
        in_specs=[pl.BlockSpec(memory_space=pl.ANY)] * 2,
        out_specs=(pl.BlockSpec(memory_space=pl.ANY),) * 3,
        scratch_shapes=[
            pltpu.VMEM((rows, ncol, lane), f32),
            pltpu.VMEM((chunks, blocks, q, width), f32),
            pltpu.VMEM((2, lead, unit, lane), f32),
            pltpu.VMEM((bands, classes * rows, blocks * lane), bf16),
            pltpu.VMEM((bands, classes * rows, blocks * lane), bf16),
            pltpu.VMEM((blocks, lane, width), f32),
            pltpu.VMEM((blocks * lane, width), bf16),
            pltpu.VMEM((blocks * lane, width), bf16),
            pltpu.VMEM((chunks, per, classes, rows, lane), f32),
            pltpu.VMEM((chunks, per, classes - 1, rows, lane), f32),
            dma((classes,)),
            dma((classes,)),
            dma((2, chunks)),
            dma((2, chunks, spots)),
            dma((2, chunks, spots)),
            dma((chunks, spots)),
            dma((chunks, spots)),
            dma((chunks,)),
            dma((chunks, per, levels)),
            dma((chunks, per, levels)),
            dma((2,)),
            dma((1,)),
            dma((ncol // sub,)),
        ],
        compiler_params=pltpu.CompilerParams(
            collective_id=0, has_side_effects=True, vmem_limit_bytes=60 * 1024 * 1024
        ),
    )(left, right)
    out = out.reshape(rows, halves, wide // lane, cols, lane)
    return jnp.transpose(out, (0, 1, 3, 2, 4)).reshape(b_blocks.shape)


def fits(classes, subs, first_factor_tiles, b_blocks):
    blocks, q, halves, cols, order = first_factor_tiles.shape
    bands, spots = order // (LANE * classes), subs // 2
    return (
        q % SUBLANE == 0 and order % (LANE * classes) == 0 and (bands * cols) % SUBLANE == 0
        and bands * LANE == subs * q and spots % bands == 0
    )


def either(classes, subs, first_factor_tiles, b_blocks):
    pick = streamed if fits(classes, subs, first_factor_tiles, b_blocks) else local
    return pick(classes, subs, first_factor_tiles, b_blocks)


def solution(mesh):
    spec = P(None, ("cls", "str"), None, None, None)
    return jax.shard_map(
        functools.partial(either, mesh.shape["cls"], mesh.shape["str"]),
        mesh=mesh, in_specs=(spec, spec), out_specs=spec, check_vma=False,
    )
```

```python
import functools

import jax
import jax.numpy as jnp
from jax import lax
from jax.experimental import pallas as pl
from jax.experimental.pallas import tpu as pltpu
from jax.sharding import PartitionSpec as P

MESH = pl.DeviceIdType.MESH
LAG = 3
EARLY = 2
AHEAD = 6
LEAD = 2
CALM = 10
LANE = 128
SUBLANE = 8


def flip(index, mask, count):
    out, bit = index, 1
    while bit < count:
        have, want = (index // bit) % 2, (mask // bit) % 2
        out = out + want * (1 - 2 * have) * bit
        bit *= 2
    return out


def kernel(
    classes, subs, a_ref, b_ref, o_ref, aland, ball,
    ahi, alo, astage, bstage, bhi, blo, cpart, rland,
    a_send, a_recv, own_send, fwd_send, line_recv, peer_send, peer_recv,
    c_send, c_recv, a_load, b_load, o_sem,
):
    chunks, groups, piece, width = b_ref.shape
    rows = a_ref.shape[1]
    depth = subs * piece
    spots = subs // 2
    c, s = lax.axis_index("cls"), lax.axis_index("str")
    spot, core = s // 2, s % 2
    mate = (c, s + 1 - 2 * core)
    beside = ((c, s - 2), (c, s + 2))
    has = (spot > 0, spot < spots - 1)

    barrier = pltpu.get_barrier_semaphore()
    for d in range(1, classes):
        pl.semaphore_signal(barrier, inc=1, device_id=(flip(c, d, classes), s), device_id_type=MESH)
    pl.semaphore_signal(barrier, inc=1, device_id=mate, device_id_type=MESH)
    for side in range(2):
        @pl.when(has[side])
        def _():
            pl.semaphore_signal(barrier, inc=1, device_id=beside[side], device_id_type=MESH)
    lower, higher = (spot + spots - 1) // spots, (2 * spots - 2 - spot) // spots
    pl.semaphore_wait(barrier, classes + lower + higher)

    def remote(src, dst, send, recv, to):
        return pltpu.make_async_remote_copy(
            src_ref=src, dst_ref=dst, send_sem=send, recv_sem=recv,
            device_id=to, device_id_type=MESH,
        )

    def slot(j, owner):
        return ball.at[j, :, pl.ds(pl.multiple_of(owner * piece, piece), piece), :]

    def own_line(j, side):
        return remote(b_ref.at[j], slot(j, s), own_send.at[side, j], line_recv.at[side, j, 0], beside[side])

    def own_mate(j):
        return remote(b_ref.at[j], slot(j, s), peer_send.at[j, spot], peer_recv.at[j, spot], mate)

    def origin(side, dist):
        return spot + dist if side == 0 else spot - dist

    def there(side, dist):
        return spot + dist < spots if side == 0 else spot >= dist

    def arrival(j, side, dist):
        at = slot(j, 2 * origin(side, dist) + core)
        return remote(at, at, own_send.at[side, j], line_recv.at[side, j, dist - 1], beside[1 - side])

    def onward(j, side, dist):
        at = slot(j, 2 * origin(side, dist) + core)
        return remote(at, at, fwd_send.at[side, j, dist - 1], line_recv.at[side, j, dist], beside[side])

    def across(j, side, dist):
        begin = origin(side, dist)
        at = slot(j, 2 * begin + core)
        return remote(at, at, peer_send.at[j, begin], peer_recv.at[j, begin], mate)

    def forward(j, dist):
        for side in range(2):
            @pl.when(there(side, dist))
            def _():
                arrival(j, side, dist).wait_recv()

                @pl.when(has[side])
                def _():
                    onward(j, side, dist).start()

                across(j, side, dist).start()

    def a_copy(d):
        peer = flip(c, d, classes)
        return remote(
            a_ref.at[:, :, pl.ds(pl.multiple_of(peer * depth, depth), depth)],
            aland.at[:, pl.ds(pl.multiple_of(c * rows, rows), rows), :],
            a_send.at[d], a_recv.at[d], (peer, s),
        )

    for d in range(1, classes):
        a_copy(d).start()

    def begin(j, _):
        for side in range(2):
            @pl.when(has[side])
            def _():
                own_line(j, side).start()
        own_mate(j).start()
        return 0

    lax.fori_loop(0, chunks, begin, 0)

    for j in range(min(EARLY, chunks)):
        forward(j, 1)
    for d in range(1, classes):
        a_copy(d).wait_recv()

    def load_a(g, held):
        for e in range(classes):
            to = astage.at[held, pl.ds(e * rows, rows), :]

            @pl.when(c == e)
            def _():
                pltpu.make_async_copy(
                    a_ref.at[g, :, pl.ds(pl.multiple_of(c * depth, depth), depth)], to, a_load.at[held]
                ).start()

            @pl.when(c != e)
            def _():
                pltpu.make_async_copy(aland.at[g, pl.ds(e * rows, rows), :], to, a_load.at[held]).start()

    load_a(0, 0)
    for g in range(groups):
        held = g % 2
        if g + 1 < groups:
            load_a(g + 1, 1 - held)
        pltpu.make_async_copy(aland.at[g], astage.at[held], a_load.at[held]).wait()

        def split(m, _, held=held, g=g):
            at = pl.ds(pl.multiple_of(m * rows, rows), rows)
            value = astage[held, at, :]
            high = value.astype(jnp.bfloat16)
            ahi[at, g * depth:(g + 1) * depth] = high
            alo[at, g * depth:(g + 1) * depth] = (value - high.astype(jnp.float32)).astype(jnp.bfloat16)
            return 0

        lax.fori_loop(0, classes, split, 0)

    def c_copy(j, d):
        peer = flip(c, d, classes)
        return remote(
            cpart.at[j, pl.ds(pl.multiple_of(peer * rows, rows), rows), :],
            rland.at[j, d - 1], c_send.at[j, d], c_recv.at[j, d], (peer, s),
        )

    mine = pl.ds(pl.multiple_of(c * rows, rows), rows)

    def out_copy(j):
        return pltpu.make_async_copy(cpart.at[j, mine, :], o_ref.at[j], o_sem.at[j])

    def reduce(j):
        for d in range(1, classes):
            c_copy(j, d).wait_recv()
        total = cpart[j, mine, :]
        for d in range(1, classes):
            total = total + rland[j, d - 1]
        cpart[j, mine, :] = total
        out_copy(j).start()

    def step(j, _):
        if spots > 1:
            @pl.when(j + EARLY < chunks)
            def _():
                forward(j + EARLY, 1)
        for dist in range(2, spots):
            forward(j, dist)

        for owner in range(subs):
            to = bstage.at[:, pl.ds(owner * piece, piece), :]

            @pl.when(s == owner)
            def _():
                pltpu.make_async_copy(b_ref.at[j], to, b_load.at[0]).start()

            @pl.when(s != owner)
            def _():
                @pl.when(core != owner % 2)
                def _():
                    remote(to_slot(j, owner), to_slot(j, owner), peer_send.at[j, owner // 2],
                           peer_recv.at[j, owner // 2], mate).wait_recv()

                pltpu.make_async_copy(to_slot(j, owner), to, b_load.at[0]).start()

        pltpu.make_async_copy(ball.at[j], bstage, b_load.at[0]).wait()

        def split(g, _):
            value = bstage[g]
            high = value.astype(jnp.bfloat16)
            at = pl.ds(pl.multiple_of(g * depth, depth), depth)
            bhi[at, :] = high
            blo[at, :] = (value - high.astype(jnp.float32)).astype(jnp.bfloat16)
            return 0

        lax.fori_loop(0, groups, split, 0)

        def part(i, _):
            d = (i + 1) % classes
            at = pl.ds(pl.multiple_of(flip(c, d, classes) * rows, rows), rows)
            dot = functools.partial(jnp.dot, preferred_element_type=jnp.float32)
            cpart[j, at, :] = (
                dot(ahi[at, :], bhi[...]) + dot(ahi[at, :], blo[...]) + dot(alo[at, :], bhi[...])
            )

            @pl.when(d != 0)
            def _():
                c_copy(j, d).start()

            return 0

        lax.fori_loop(0, classes, part, 0)

        @pl.when(j >= LAG)
        def _():
            reduce(j - LAG)

        return 0

    def to_slot(j, owner):
        return ball.at[j, :, pl.ds(owner * piece, piece), :]

    lax.fori_loop(0, chunks, step, 0)
    for j in range(max(chunks - LAG, 0), chunks):
        reduce(j)

    def finish(j, _):
        out_copy(j).wait()
        own_mate(j).wait_send()
        for d in range(1, classes):
            c_copy(j, d).wait_send()
        for side in range(2):
            @pl.when(has[side])
            def _():
                own_line(j, side).wait_send()
            for dist in range(1, spots):
                @pl.when(there(side, dist))
                def _():
                    @pl.when(has[side])
                    def _():
                        onward(j, side, dist).wait_send()
                    across(j, side, dist).wait_send()
        return 0

    lax.fori_loop(0, chunks, finish, 0)
    for d in range(1, classes):
        a_copy(d).wait_send()


def local(classes, subs, first_factor_tiles, b_blocks):
    blocks, q, halves, cols, order = first_factor_tiles.shape
    inner, width = halves * cols, b_blocks.shape[4]
    rows = blocks * q
    left = first_factor_tiles.reshape(rows, inner, order)
    right = jnp.transpose(b_blocks.reshape(inner, q, inner, width), (2, 0, 1, 3))
    if q % 8 == 0:
        left = jnp.transpose(left, (1, 0, 2))
    else:
        left = left.reshape(rows, inner, classes * subs, q)
        left = jnp.transpose(left, (0, 2, 1, 3)).reshape(1, rows, inner * order)
        right = right.reshape(inner, 1, inner * q, width)
    chunks, groups, piece, _ = right.shape
    depth = subs * piece
    dma = pltpu.SemaphoreType.DMA
    f32, bf16 = jnp.float32, jnp.bfloat16
    spots = subs // 2
    out, _, _ = pl.pallas_call(
        functools.partial(kernel, classes, subs),
        out_shape=(
            jax.ShapeDtypeStruct((chunks, rows, width), f32),
            jax.ShapeDtypeStruct((groups, classes * rows, depth), f32),
            jax.ShapeDtypeStruct((chunks, groups, depth, width), f32),
        ),
        in_specs=[pl.BlockSpec(memory_space=pl.ANY)] * 2,
        out_specs=(pl.BlockSpec(memory_space=pl.ANY),) * 3,
        scratch_shapes=[
            pltpu.VMEM((classes * rows, groups * depth), bf16),
            pltpu.VMEM((classes * rows, groups * depth), bf16),
            pltpu.VMEM((2, classes * rows, depth), f32),
            pltpu.VMEM((groups, depth, width), f32),
            pltpu.VMEM((groups * depth, width), bf16),
            pltpu.VMEM((groups * depth, width), bf16),
            pltpu.VMEM((chunks, classes * rows, width), f32),
            pltpu.VMEM((chunks, classes - 1, rows, width), f32),
            dma((classes,)),
            dma((classes,)),
            dma((2, chunks)),
            dma((2, chunks, spots)),
            dma((2, chunks, spots)),
            dma((chunks, spots)),
            dma((chunks, spots)),
            dma((chunks, classes)),
            dma((chunks, classes)),
            dma((2,)),
            dma((1,)),
            dma((chunks,)),
        ],
        compiler_params=pltpu.CompilerParams(
            collective_id=0, has_side_effects=True, vmem_limit_bytes=60 * 1024 * 1024
        ),
    )(left, right)
    out = jnp.transpose(out, (1, 0, 2))
    return out.reshape(b_blocks.shape)


def stream(
    classes, subs, a_ref, b_ref, o_ref, aland, ball,
    flat, bown, astage, ahi, alo, bstage, bhi, blo, cpart, rland,
    a_send, a_recv, own_send, fwd_send, line_recv, peer_send, peer_recv, keep_sem,
    c_send, c_recv, a_load, b_load, o_sem,
):
    lead, _, unit, lane = a_ref.shape
    rows, ncol, _ = b_ref.shape
    chunks, blocks, depth, width = ball.shape
    bands = depth // lane
    piece = depth // subs
    per = width // lane
    levels = classes.bit_length() - 1
    spots = subs // 2
    c, s = lax.axis_index("cls"), lax.axis_index("str")
    spot, core = s // 2, s % 2
    mate = (c, s + 1 - 2 * core)
    beside = ((c, s - 2), (c, s + 2))
    has = (spot > 0, spot < spots - 1)
    inner = (spot > 0) & (spot < spots - 1)
    outer = (spot == 0) | (spot == spots - 1)
    near = spot // (spots // bands)

    barrier = pltpu.get_barrier_semaphore()
    for d in range(1, classes):
        pl.semaphore_signal(barrier, inc=1, device_id=(flip(c, d, classes), s), device_id_type=MESH)
    pl.semaphore_signal(barrier, inc=1, device_id=mate, device_id_type=MESH)
    for side in range(2):
        @pl.when(has[side])
        def _():
            pl.semaphore_signal(barrier, inc=1, device_id=beside[side], device_id_type=MESH)
    b_in = pltpu.make_async_copy(b_ref, flat, b_load.at[0])
    b_in.start()
    lower, higher = (spot + spots - 1) // spots, (2 * spots - 2 - spot) // spots
    pl.semaphore_wait(barrier, classes + lower + higher)

    def remote(src, dst, send, recv, to):
        return pltpu.make_async_remote_copy(
            src_ref=src, dst_ref=dst, send_sem=send, recv_sem=recv,
            device_id=to, device_id_type=MESH,
        )

    def a_copy(d):
        peer = flip(c, d, classes)
        return remote(a_ref.at[:, peer], aland.at[d - 1], a_send.at[d], a_recv.at[d], (peer, s))

    for d in range(1, classes):
        a_copy(d).start()

    def slot(j, owner):
        return ball.at[j, :, pl.ds(pl.multiple_of(owner * piece, piece), piece), :]

    def own_line(j, side):
        return remote(bown.at[j], slot(j, s), own_send.at[side, j], line_recv.at[side, j, 0], beside[side])

    def own_mate(j):
        return remote(bown.at[j], slot(j, s), peer_send.at[j, spot], peer_recv.at[j, spot], mate)

    def own_keep(j):
        return pltpu.make_async_copy(bown.at[j], slot(j, s), keep_sem.at[j])

    def origin(side, dist):
        return spot + dist if side == 0 else spot - dist

    def there(side, dist):
        return spot + dist < spots if side == 0 else spot >= dist

    def arrival(j, side, dist):
        at = slot(j, 2 * origin(side, dist) + core)
        return remote(at, at, own_send.at[side, j], line_recv.at[side, j, dist - 1], beside[1 - side])

    def onward(j, side, dist):
        at = slot(j, 2 * origin(side, dist) + core)
        return remote(at, at, fwd_send.at[side, j, dist - 1], line_recv.at[side, j, dist], beside[side])

    def across(j, side, dist):
        begin = origin(side, dist)
        at = slot(j, 2 * begin + core)
        return remote(at, at, peer_send.at[j, begin], peer_recv.at[j, begin], mate)

    def forward(j, dist):
        for side in range(2):
            @pl.when(there(side, dist))
            def _():
                arrival(j, side, dist).wait_recv()

                @pl.when(has[side])
                def _():
                    onward(j, side, dist).start()

                across(j, side, dist).start()

    def own_out(j):
        for side in range(2):
            @pl.when(has[side])
            def _():
                own_line(j, side).start()

    b_in.wait()
    rows_of = flat.reshape(rows * ncol, lane)

    def lay(j):
        for p in range(per):
            value = rows_of[pl.ds(j * per + p, rows, stride=ncol), :]
            bown[j, :, :, p * lane:(p + 1) * lane] = value.reshape(blocks, piece, lane)

    for j in range(min(LEAD, chunks)):
        lay(j)
    for j in range(min(LEAD, chunks)):
        own_out(j)

    def lay_more(j, _):
        lay(j)
        return 0

    lax.fori_loop(min(LEAD, chunks), chunks, lay_more, 0)

    def begin(j, _):
        own_mate(j).start()
        own_keep(j).start()

        @pl.when(outer & (j >= LEAD))
        def _():
            own_out(j)

        return 0

    lax.fori_loop(0, chunks, begin, 0)

    def take_a(d):
        held = astage.at[d % 2]
        if d == 0:
            return pltpu.make_async_copy(a_ref.at[:, c], held, a_load.at[0])
        return pltpu.make_async_copy(aland.at[d - 1], held, a_load.at[d % 2])

    def split_a(d):
        lines = astage.at[d % 2].reshape(lead * unit, lane)
        stride = lead * unit // rows
        cols = unit // bands

        def one(k, _):
            h, band, col = k // unit, (k % unit) // cols, k % cols
            value = lines[pl.ds(k, rows, stride=stride), :]
            high = value.astype(jnp.bfloat16)
            at = pl.ds(pl.multiple_of((h * cols + col) * lane, lane), lane)
            ahi[band, d * rows:(d + 1) * rows, at] = high
            alo[band, d * rows:(d + 1) * rows, at] = (value - high.astype(jnp.float32)).astype(jnp.bfloat16)
            return 0

        lax.fori_loop(0, stride, one, 0)

    take_a(0).start()
    take_a(0).wait()
    split_a(0)

    @pl.when(inner)
    def _():
        def early(j, _):
            for dist in range(1, spots):
                forward(j, dist)

            @pl.when(j + LEAD < chunks)
            def _():
                own_out(j + LEAD)

            return 0

        lax.fori_loop(0, min(AHEAD, chunks), early, 0)

    for d in range(1, classes):
        a_copy(d).wait_recv()
        take_a(d).start()
        if d > 1:
            take_a(d - 1).wait()
            split_a(d - 1)
    take_a(classes - 1).wait()
    split_a(classes - 1)

    def order(p):
        return [(p + i) % levels for i in range(levels)]

    def place(p, d):
        at = 0
        for bit in order(p):
            at = 2 * at + (d // (1 << bit)) % 2
        return at

    def c_copy(j, p, level):
        count = classes >> (level + 1)
        peer = flip(c, 1 << order(p)[level], classes)
        return remote(
            cpart.at[j, p, pl.ds(count, count)],
            rland.at[j, p, pl.ds(classes - 2 * count, count)],
            c_send.at[j, p, level], c_recv.at[j, p, level], (peer, s),
        )

    share = ncol // o_sem.shape[0]

    def out_copy(g):
        at = pl.ds(pl.multiple_of(g * share, share), share)
        return pltpu.make_async_copy(flat.at[:, at, :], o_ref.at[:, at, :], o_sem.at[g])

    def reduce(j, level):
        count = classes >> (level + 1)
        for p in range(per):
            c_copy(j, p, level).wait_recv()
            if level + 1 < levels:
                cpart[j, p, 0:count] = (
                    cpart[j, p, 0:count] + rland[j, p, classes - 2 * count:classes - count]
                )
                c_copy(j, p, level + 1).start()
            else:
                rows_of[pl.ds(j * per + p, rows, stride=ncol), :] = (
                    cpart[j, p, 0] + rland[j, p, classes - 2]
                )
        if level + 1 == levels:
            @pl.when((j + 1) % (share // per) == 0)
            def _():
                out_copy((j + 1) // (share // per) - 1).start()

    def gather(j, band):
        for owner in range(subs):
            @pl.when(owner // (subs // bands) == band)
            def _():
                @pl.when(s == owner)
                def _():
                    own_keep(j).wait()

                @pl.when(core != owner % 2)
                def _():
                    at = slot(j, owner)
                    remote(at, at, peer_send.at[j, owner // 2], peer_recv.at[j, owner // 2], mate).wait_recv()

    def take_b(j, band, held):
        at = pl.ds(pl.multiple_of(band * lane, lane), lane)
        return pltpu.make_async_copy(ball.at[j, :, at, :], bstage.at[held], b_load.at[held])

    def split_b(held):
        def split(g, _):
            value = bstage[held, g]
            high = value.astype(jnp.bfloat16)
            at = pl.ds(pl.multiple_of(g * lane, lane), lane)
            bhi[at, :] = high
            blo[at, :] = (value - high.astype(jnp.float32)).astype(jnp.bfloat16)
            return 0

        lax.fori_loop(0, blocks, split, 0)

    def multiply(j, band, first):
        dot = functools.partial(jnp.dot, preferred_element_type=jnp.float32)

        def part(d, _):
            at = pl.ds(pl.multiple_of(d * rows, rows), rows)
            high, low = ahi[band, at, :], alo[band, at, :]
            total = dot(high, bhi[...]) + dot(high, blo[...]) + dot(low, bhi[...])
            for p in range(per):
                value = total[:, p * lane:(p + 1) * lane]
                to = place(p, d)
                cpart[j, p, to] = value if first else cpart[j, p, to] + value
            return 0

        lax.fori_loop(0, classes, part, 0)

    def sum_first(k, _):
        reduce(k, 0)
        return 0

    def sum_rest(k, _):
        for level in range(1, levels):
            reduce(k, level)
        return 0

    calm = jnp.where(outer, chunks * CALM // 16, chunks)

    def first_sums(j):
        return jnp.where(j > calm, j, jnp.maximum(j - 1, 0))

    def last_sums(j):
        return jnp.where(j > calm, j, jnp.maximum(j - 2, 0))

    def step(j, _):
        @pl.when(inner & (j + AHEAD < chunks))
        def _():
            for dist in range(1, spots):
                forward(j + AHEAD, dist)

            @pl.when(j + AHEAD + LEAD < chunks)
            def _():
                own_out(j + AHEAD + LEAD)

        @pl.when(outer)
        def _():
            forward(j, 1)

        gather(j, near)
        take_b(j, near, 0).start()
        lax.fori_loop(first_sums(j - 1), first_sums(j), sum_first, 0)
        take_b(j, near, 0).wait()
        split_b(0)
        multiply(j, near, True)

        @pl.when(outer)
        def _():
            for dist in range(2, spots):
                forward(j, dist)

        for k in range(1, bands):
            band = (near + k) % bands
            gather(j, band)
            take_b(j, band, k % 2).start()
            if k == 1:
                lax.fori_loop(last_sums(j - 1), last_sums(j), sum_rest, 0)
            take_b(j, band, k % 2).wait()
            split_b(k % 2)
            multiply(j, band, False)
        for p in range(per):
            c_copy(j, p, 0).start()
        return 0

    lax.fori_loop(0, chunks, step, 0)
    lax.fori_loop(first_sums(chunks - 1), chunks, sum_first, 0)
    lax.fori_loop(last_sums(chunks - 1), chunks, sum_rest, 0)
    for g in range(o_sem.shape[0]):
        out_copy(g).wait()

    def finish(j, _):
        own_mate(j).wait_send()
        for p in range(per):
            for level in range(levels):
                c_copy(j, p, level).wait_send()
        for side in range(2):
            @pl.when(has[side])
            def _():
                own_line(j, side).wait_send()
            for dist in range(1, spots):
                @pl.when(there(side, dist))
                def _():
                    @pl.when(has[side])
                    def _():
                        onward(j, side, dist).wait_send()
                    across(j, side, dist).wait_send()
        return 0

    lax.fori_loop(0, chunks, finish, 0)
    for d in range(1, classes):
        a_copy(d).wait_send()


def streamed(classes, subs, first_factor_tiles, b_blocks):
    blocks, q, halves, cols, order = first_factor_tiles.shape
    wide = b_blocks.shape[4]
    lane, sub = LANE, SUBLANE
    rows, bands, ncol = blocks * q, order // (LANE * classes), halves * cols * wide // LANE
    left = first_factor_tiles.reshape(rows, halves, cols, classes * bands, lane)
    left = jnp.transpose(left, (0, 1, 3, 2, 4)).reshape(rows * halves, classes, bands * cols, lane)
    right = b_blocks.reshape(rows, halves, cols, wide // lane, lane)
    right = jnp.transpose(right, (0, 1, 3, 2, 4)).reshape(rows, ncol, lane)
    lead, unit = rows * halves, bands * cols
    per = 2
    chunks, width, depth = ncol // per, per * lane, bands * lane
    dma = pltpu.SemaphoreType.DMA
    f32, bf16 = jnp.float32, jnp.bfloat16
    spots, levels = subs // 2, classes.bit_length() - 1
    out, _, _ = pl.pallas_call(
        functools.partial(stream, classes, subs),
        out_shape=(
            jax.ShapeDtypeStruct((rows, ncol, lane), f32),
            jax.ShapeDtypeStruct((classes - 1, lead, unit, lane), f32),
            jax.ShapeDtypeStruct((chunks, blocks, depth, width), f32),
        ),
        in_specs=[pl.BlockSpec(memory_space=pl.ANY)] * 2,
        out_specs=(pl.BlockSpec(memory_space=pl.ANY),) * 3,
        scratch_shapes=[
            pltpu.VMEM((rows, ncol, lane), f32),
            pltpu.VMEM((chunks, blocks, q, width), f32),
            pltpu.VMEM((2, lead, unit, lane), f32),
            pltpu.VMEM((bands, classes * rows, blocks * lane), bf16),
            pltpu.VMEM((bands, classes * rows, blocks * lane), bf16),
            pltpu.VMEM((2, blocks, lane, width), f32),
            pltpu.VMEM((blocks * lane, width), bf16),
            pltpu.VMEM((blocks * lane, width), bf16),
            pltpu.VMEM((chunks, per, classes, rows, lane), f32),
            pltpu.VMEM((chunks, per, classes - 1, rows, lane), f32),
            dma((classes,)),
            dma((classes,)),
            dma((2, chunks)),
            dma((2, chunks, spots)),
            dma((2, chunks, spots)),
            dma((chunks, spots)),
            dma((chunks, spots)),
            dma((chunks,)),
            dma((chunks, per, levels)),
            dma((chunks, per, levels)),
            dma((2,)),
            dma((2,)),
            dma((ncol // sub,)),
        ],
        compiler_params=pltpu.CompilerParams(
            collective_id=0, has_side_effects=True, vmem_limit_bytes=60 * 1024 * 1024
        ),
    )(left, right)
    out = out.reshape(rows, halves, wide // lane, cols, lane)
    return jnp.transpose(out, (0, 1, 3, 2, 4)).reshape(b_blocks.shape)


def fits(classes, subs, first_factor_tiles, b_blocks):
    blocks, q, halves, cols, order = first_factor_tiles.shape
    bands, spots = order // (LANE * classes), subs // 2
    return (
        classes > 1 and bands > 1 and q % SUBLANE == 0 and order % (LANE * classes) == 0 and (bands * cols) % SUBLANE == 0
        and bands * LANE == subs * q and spots % bands == 0
    )


def either(classes, subs, first_factor_tiles, b_blocks):
    pick = streamed if fits(classes, subs, first_factor_tiles, b_blocks) else local
    return pick(classes, subs, first_factor_tiles, b_blocks)


def solution(mesh):
    spec = P(None, ("cls", "str"), None, None, None)
    return jax.shard_map(
        functools.partial(either, mesh.shape["cls"], mesh.shape["str"]),
        mesh=mesh, in_specs=(spec, spec), out_specs=spec, check_vma=False,
    )
```

```python
import functools

import jax
import jax.numpy as jnp
from jax import lax
from jax.experimental import pallas as pl
from jax.experimental.pallas import tpu as pltpu
from jax.sharding import PartitionSpec as P

MESH = pl.DeviceIdType.MESH
LAG = 3
EARLY = 2
AHEAD = 7
LEAD = 2
MORE = 2
GIVEN = 2
SLOTS = 8
CALM = 14
LANE = 128
SUBLANE = 8


def flip(index, mask, count):
    out, bit = index, 1
    while bit < count:
        have, want = (index // bit) % 2, (mask // bit) % 2
        out = out + want * (1 - 2 * have) * bit
        bit *= 2
    return out


def kernel(
    classes, subs, a_ref, b_ref, o_ref, aland, ball,
    ahi, alo, astage, bstage, bhi, blo, cpart, rland,
    a_send, a_recv, own_send, fwd_send, line_recv, peer_send, peer_recv,
    c_send, c_recv, a_load, b_load, o_sem,
):
    chunks, groups, piece, width = b_ref.shape
    rows = a_ref.shape[1]
    depth = subs * piece
    spots = subs // 2
    c, s = lax.axis_index("cls"), lax.axis_index("str")
    spot, core = s // 2, s % 2
    mate = (c, s + 1 - 2 * core)
    beside = ((c, s - 2), (c, s + 2))
    has = (spot > 0, spot < spots - 1)

    barrier = pltpu.get_barrier_semaphore()
    for d in range(1, classes):
        pl.semaphore_signal(barrier, inc=1, device_id=(flip(c, d, classes), s), device_id_type=MESH)
    pl.semaphore_signal(barrier, inc=1, device_id=mate, device_id_type=MESH)
    for side in range(2):
        @pl.when(has[side])
        def _():
            pl.semaphore_signal(barrier, inc=1, device_id=beside[side], device_id_type=MESH)
    lower, higher = (spot + spots - 1) // spots, (2 * spots - 2 - spot) // spots
    pl.semaphore_wait(barrier, classes + lower + higher)

    def remote(src, dst, send, recv, to):
        return pltpu.make_async_remote_copy(
            src_ref=src, dst_ref=dst, send_sem=send, recv_sem=recv,
            device_id=to, device_id_type=MESH,
        )

    def slot(j, owner):
        return ball.at[j, :, pl.ds(pl.multiple_of(owner * piece, piece), piece), :]

    def own_line(j, side):
        return remote(b_ref.at[j], slot(j, s), own_send.at[side, j], line_recv.at[side, j, 0], beside[side])

    def own_mate(j):
        return remote(b_ref.at[j], slot(j, s), peer_send.at[j, spot], peer_recv.at[j, spot], mate)

    def origin(side, dist):
        return spot + dist if side == 0 else spot - dist

    def there(side, dist):
        return spot + dist < spots if side == 0 else spot >= dist

    def arrival(j, side, dist):
        at = slot(j, 2 * origin(side, dist) + core)
        return remote(at, at, own_send.at[side, j], line_recv.at[side, j, dist - 1], beside[1 - side])

    def onward(j, side, dist):
        at = slot(j, 2 * origin(side, dist) + core)
        return remote(at, at, fwd_send.at[side, j, dist - 1], line_recv.at[side, j, dist], beside[side])

    def across(j, side, dist):
        begin = origin(side, dist)
        at = slot(j, 2 * begin + core)
        return remote(at, at, peer_send.at[j, begin], peer_recv.at[j, begin], mate)

    def forward(j, dist):
        for side in range(2):
            @pl.when(there(side, dist))
            def _():
                arrival(j, side, dist).wait_recv()

                @pl.when(has[side])
                def _():
                    onward(j, side, dist).start()

                across(j, side, dist).start()

    def a_copy(d):
        peer = flip(c, d, classes)
        return remote(
            a_ref.at[:, :, pl.ds(pl.multiple_of(peer * depth, depth), depth)],
            aland.at[:, pl.ds(pl.multiple_of(c * rows, rows), rows), :],
            a_send.at[d], a_recv.at[d], (peer, s),
        )

    for d in range(1, classes):
        a_copy(d).start()

    def begin(j, _):
        for side in range(2):
            @pl.when(has[side])
            def _():
                own_line(j, side).start()
        own_mate(j).start()
        return 0

    lax.fori_loop(0, chunks, begin, 0)

    for j in range(min(EARLY, chunks)):
        forward(j, 1)
    for d in range(1, classes):
        a_copy(d).wait_recv()

    def load_a(g, held):
        for e in range(classes):
            to = astage.at[held, pl.ds(e * rows, rows), :]

            @pl.when(c == e)
            def _():
                pltpu.make_async_copy(
                    a_ref.at[g, :, pl.ds(pl.multiple_of(c * depth, depth), depth)], to, a_load.at[held]
                ).start()

            @pl.when(c != e)
            def _():
                pltpu.make_async_copy(aland.at[g, pl.ds(e * rows, rows), :], to, a_load.at[held]).start()

    load_a(0, 0)
    for g in range(groups):
        held = g % 2
        if g + 1 < groups:
            load_a(g + 1, 1 - held)
        pltpu.make_async_copy(aland.at[g], astage.at[held], a_load.at[held]).wait()

        def split(m, _, held=held, g=g):
            at = pl.ds(pl.multiple_of(m * rows, rows), rows)
            value = astage[held, at, :]
            high = value.astype(jnp.bfloat16)
            ahi[at, g * depth:(g + 1) * depth] = high
            alo[at, g * depth:(g + 1) * depth] = (value - high.astype(jnp.float32)).astype(jnp.bfloat16)
            return 0

        lax.fori_loop(0, classes, split, 0)

    def c_copy(j, d):
        peer = flip(c, d, classes)
        return remote(
            cpart.at[j, pl.ds(pl.multiple_of(peer * rows, rows), rows), :],
            rland.at[j, d - 1], c_send.at[j, d], c_recv.at[j, d], (peer, s),
        )

    mine = pl.ds(pl.multiple_of(c * rows, rows), rows)

    def out_copy(j):
        return pltpu.make_async_copy(cpart.at[j, mine, :], o_ref.at[j], o_sem.at[j])

    def reduce(j):
        for d in range(1, classes):
            c_copy(j, d).wait_recv()
        total = cpart[j, mine, :]
        for d in range(1, classes):
            total = total + rland[j, d - 1]
        cpart[j, mine, :] = total
        out_copy(j).start()

    def step(j, _):
        if spots > 1:
            @pl.when(j + EARLY < chunks)
            def _():
                forward(j + EARLY, 1)
        for dist in range(2, spots):
            forward(j, dist)

        for owner in range(subs):
            to = bstage.at[:, pl.ds(owner * piece, piece), :]

            @pl.when(s == owner)
            def _():
                pltpu.make_async_copy(b_ref.at[j], to, b_load.at[0]).start()

            @pl.when(s != owner)
            def _():
                @pl.when(core != owner % 2)
                def _():
                    remote(to_slot(j, owner), to_slot(j, owner), peer_send.at[j, owner // 2],
                           peer_recv.at[j, owner // 2], mate).wait_recv()

                pltpu.make_async_copy(to_slot(j, owner), to, b_load.at[0]).start()

        pltpu.make_async_copy(ball.at[j], bstage, b_load.at[0]).wait()

        def split(g, _):
            value = bstage[g]
            high = value.astype(jnp.bfloat16)
            at = pl.ds(pl.multiple_of(g * depth, depth), depth)
            bhi[at, :] = high
            blo[at, :] = (value - high.astype(jnp.float32)).astype(jnp.bfloat16)
            return 0

        lax.fori_loop(0, groups, split, 0)

        def part(i, _):
            d = (i + 1) % classes
            at = pl.ds(pl.multiple_of(flip(c, d, classes) * rows, rows), rows)
            dot = functools.partial(jnp.dot, preferred_element_type=jnp.float32)
            cpart[j, at, :] = (
                dot(ahi[at, :], bhi[...]) + dot(ahi[at, :], blo[...]) + dot(alo[at, :], bhi[...])
            )

            @pl.when(d != 0)
            def _():
                c_copy(j, d).start()

            return 0

        lax.fori_loop(0, classes, part, 0)

        @pl.when(j >= LAG)
        def _():
            reduce(j - LAG)

        return 0

    def to_slot(j, owner):
        return ball.at[j, :, pl.ds(owner * piece, piece), :]

    lax.fori_loop(0, chunks, step, 0)
    for j in range(max(chunks - LAG, 0), chunks):
        reduce(j)

    def finish(j, _):
        out_copy(j).wait()
        own_mate(j).wait_send()
        for d in range(1, classes):
            c_copy(j, d).wait_send()
        for side in range(2):
            @pl.when(has[side])
            def _():
                own_line(j, side).wait_send()
            for dist in range(1, spots):
                @pl.when(there(side, dist))
                def _():
                    @pl.when(has[side])
                    def _():
                        onward(j, side, dist).wait_send()
                    across(j, side, dist).wait_send()
        return 0

    lax.fori_loop(0, chunks, finish, 0)
    for d in range(1, classes):
        a_copy(d).wait_send()


def local(classes, subs, first_factor_tiles, b_blocks):
    blocks, q, halves, cols, order = first_factor_tiles.shape
    inner, width = halves * cols, b_blocks.shape[4]
    rows = blocks * q
    left = first_factor_tiles.reshape(rows, inner, order)
    right = jnp.transpose(b_blocks.reshape(inner, q, inner, width), (2, 0, 1, 3))
    if q % 8 == 0:
        left = jnp.transpose(left, (1, 0, 2))
    else:
        left = left.reshape(rows, inner, classes * subs, q)
        left = jnp.transpose(left, (0, 2, 1, 3)).reshape(1, rows, inner * order)
        right = right.reshape(inner, 1, inner * q, width)
    chunks, groups, piece, _ = right.shape
    depth = subs * piece
    dma = pltpu.SemaphoreType.DMA
    f32, bf16 = jnp.float32, jnp.bfloat16
    spots = subs // 2
    out, _, _ = pl.pallas_call(
        functools.partial(kernel, classes, subs),
        out_shape=(
            jax.ShapeDtypeStruct((chunks, rows, width), f32),
            jax.ShapeDtypeStruct((groups, classes * rows, depth), f32),
            jax.ShapeDtypeStruct((chunks, groups, depth, width), f32),
        ),
        in_specs=[pl.BlockSpec(memory_space=pl.ANY)] * 2,
        out_specs=(pl.BlockSpec(memory_space=pl.ANY),) * 3,
        scratch_shapes=[
            pltpu.VMEM((classes * rows, groups * depth), bf16),
            pltpu.VMEM((classes * rows, groups * depth), bf16),
            pltpu.VMEM((2, classes * rows, depth), f32),
            pltpu.VMEM((groups, depth, width), f32),
            pltpu.VMEM((groups * depth, width), bf16),
            pltpu.VMEM((groups * depth, width), bf16),
            pltpu.VMEM((chunks, classes * rows, width), f32),
            pltpu.VMEM((chunks, classes - 1, rows, width), f32),
            dma((classes,)),
            dma((classes,)),
            dma((2, chunks)),
            dma((2, chunks, spots)),
            dma((2, chunks, spots)),
            dma((chunks, spots)),
            dma((chunks, spots)),
            dma((chunks, classes)),
            dma((chunks, classes)),
            dma((2,)),
            dma((1,)),
            dma((chunks,)),
        ],
        compiler_params=pltpu.CompilerParams(
            collective_id=0, has_side_effects=True, vmem_limit_bytes=60 * 1024 * 1024
        ),
    )(left, right)
    out = jnp.transpose(out, (1, 0, 2))
    return out.reshape(b_blocks.shape)


def stream(
    classes, subs, given, a_ref, b_ref, o_ref, aland, ball,
    flat, bown, astage, ahi, alo, bstage, bhi, blo, cpart, rland, lent, hhi, hlo, back,
    a_send, a_recv, lend_send, lend_recv, back_send, back_recv, own_send, fwd_send, line_recv, peer_send, peer_recv, keep_sem,
    c_send, c_recv, a_load, b_load, o_sem,
):
    lead, _, unit, lane = a_ref.shape
    rows, ncol, _ = b_ref.shape
    chunks, blocks, depth, width = ball.shape
    bands = depth // lane
    piece = depth // subs
    per = width // lane
    levels = classes.bit_length() - 1
    spots = subs // 2
    c, s = lax.axis_index("cls"), lax.axis_index("str")
    spot, core = s // 2, s % 2
    mate = (c, s + 1 - 2 * core)
    beside = ((c, s - 2), (c, s + 2))
    has = (spot > 0, spot < spots - 1)
    inner = (spot > 0) & (spot < spots - 1)
    outer = (spot == 0) | (spot == spots - 1)
    near = spot // (spots // bands)
    slots = cpart.shape[0]
    helps = (spot == 1) | (spot == spots - 2)
    total = jnp.where(helps, chunks + given, chunks)
    ends = (spot == 1, spot == spots - 2)
    friend = (c, jnp.where((spot == 0) | (spot == spots - 2), s + 2, s - 2))

    barrier = pltpu.get_barrier_semaphore()
    for d in range(1, classes):
        pl.semaphore_signal(barrier, inc=1, device_id=(flip(c, d, classes), s), device_id_type=MESH)
    pl.semaphore_signal(barrier, inc=1, device_id=mate, device_id_type=MESH)
    for side in range(2):
        @pl.when(has[side])
        def _():
            pl.semaphore_signal(barrier, inc=1, device_id=beside[side], device_id_type=MESH)
    b_in = pltpu.make_async_copy(b_ref, flat, b_load.at[0])
    b_in.start()
    lower, higher = (spot + spots - 1) // spots, (2 * spots - 2 - spot) // spots
    pl.semaphore_wait(barrier, classes + lower + higher)

    def remote(src, dst, send, recv, to):
        return pltpu.make_async_remote_copy(
            src_ref=src, dst_ref=dst, send_sem=send, recv_sem=recv,
            device_id=to, device_id_type=MESH,
        )

    def a_copy(d):
        peer = flip(c, d, classes)
        return remote(a_ref.at[:, peer], aland.at[d - 1], a_send.at[d], a_recv.at[d], (peer, s))

    for d in range(1, classes):
        a_copy(d).start()

    def slot(j, owner):
        return ball.at[j, :, pl.ds(pl.multiple_of(owner * piece, piece), piece), :]

    def own_line(j, side):
        return remote(bown.at[j], slot(j, s), own_send.at[side, j], line_recv.at[side, j, 0], beside[side])

    def own_mate(j):
        return remote(bown.at[j], slot(j, s), peer_send.at[j, spot], peer_recv.at[j, spot], mate)

    def own_keep(j):
        return pltpu.make_async_copy(bown.at[j], slot(j, s), keep_sem.at[j])

    def origin(side, dist):
        return spot + dist if side == 0 else spot - dist

    def there(side, dist):
        return spot + dist < spots if side == 0 else spot >= dist

    def arrival(j, side, dist):
        at = slot(j, 2 * origin(side, dist) + core)
        return remote(at, at, own_send.at[side, j], line_recv.at[side, j, dist - 1], beside[1 - side])

    def onward(j, side, dist):
        at = slot(j, 2 * origin(side, dist) + core)
        return remote(at, at, fwd_send.at[side, j, dist - 1], line_recv.at[side, j, dist], beside[side])

    def across(j, side, dist):
        begin = origin(side, dist)
        at = slot(j, 2 * begin + core)
        return remote(at, at, peer_send.at[j, begin], peer_recv.at[j, begin], mate)

    def forward(j, dist):
        for side in range(2):
            @pl.when(gets(j, side, dist))
            def _():
                arrival(j, side, dist).wait_recv()

                @pl.when(feeds(j, side))
                def _():
                    onward(j, side, dist).start()

                across(j, side, dist).start()

    def relay(t):
        for dist in range(1, spots):
            @pl.when((t - dist + 1 >= 0) & (t - dist + 1 < chunks))
            def _():
                forward(t - dist + 1, dist)

    def feeds(j, side):
        return has[side] & ((j >= given) | jnp.logical_not(ends[side]))

    def gets(j, side, dist):
        return there(side, dist) & ((j >= given) | inner)

    shift = given + MORE

    def own_out(j):
        for side in range(2):
            @pl.when(has[side] & jnp.logical_not(ends[side]))
            def _():
                own_line(j, side).start()

            @pl.when(ends[side] & (j + shift < chunks))
            def _():
                own_line(j + shift, side).start()

    b_in.wait()
    rows_of = flat.reshape(rows * ncol, lane)

    def lay(j):
        for p in range(per):
            value = rows_of[pl.ds(j * per + p, rows, stride=ncol), :]
            bown[j, :, :, p * lane:(p + 1) * lane] = value.reshape(blocks, piece, lane)

    first = min(LEAD + shift, chunks)
    for j in range(first):
        lay(j)
    for side in range(2):
        for j in range(given, min(given + MORE, chunks)):
            @pl.when(ends[side])
            def _():
                own_line(j, side).start()
    for j in range(min(LEAD, chunks)):
        own_out(j)

    def lay_more(j, _):
        lay(j)
        return 0

    lax.fori_loop(first, chunks, lay_more, 0)

    def begin(j, _):
        own_mate(j).start()
        own_keep(j).start()

        @pl.when(outer & (j >= LEAD))
        def _():
            own_out(j)

        return 0

    lax.fori_loop(0, chunks, begin, 0)

    def take_a(d):
        held = astage.at[d % 2]
        if d == 0:
            return pltpu.make_async_copy(a_ref.at[:, c], held, a_load.at[0])
        return pltpu.make_async_copy(aland.at[d - 1], held, a_load.at[d % 2])

    def split_a(d):
        lines = astage.at[d % 2].reshape(lead * unit, lane)
        stride = lead * unit // rows
        cols = unit // bands

        def one(k, _):
            h, band, col = k // unit, (k % unit) // cols, k % cols
            value = lines[pl.ds(k, rows, stride=stride), :]
            high = value.astype(jnp.bfloat16)
            at = pl.ds(pl.multiple_of((h * cols + col) * lane, lane), lane)
            ahi[band, d * rows:(d + 1) * rows, at] = high
            alo[band, d * rows:(d + 1) * rows, at] = (value - high.astype(jnp.float32)).astype(jnp.bfloat16)
            return 0

        lax.fori_loop(0, stride, one, 0)

    def lend_copy(d):
        return remote(lent.at[d], lent.at[d], lend_send.at[d], lend_recv.at[d], friend)

    def lend(d):
        if not given:
            return
        lines = astage.at[d % 2].reshape(lead * unit, lane)
        stride = lead * unit // rows
        cols = unit // bands
        left = lax.broadcasted_iota(jnp.int32, (rows, lane), 1) < lane // 2
        low = spot % 2 == 1

        def block(g, band):
            return lines[pl.ds((g // cols) * unit + band * cols + g % cols, rows, stride=stride), :]

        @pl.when(outer)
        def _():
            for k in range(1, bands):
                def whole(g, _, k=k):
                    at = pl.ds(pl.multiple_of(((k - 1) * blocks + g) * lane, lane), lane)
                    lent[d, :, at] = block(g, (near + k) % bands)
                    return 0

                lax.fori_loop(0, blocks, whole, 0)

            def pair(g, _):
                one, two = block(2 * g, near), block(2 * g + 1, near)
                at = pl.ds(pl.multiple_of(((bands - 1) * blocks + g) * lane, lane), lane)
                lent[d, :, at] = jnp.where(
                    left,
                    jnp.where(low, one, pltpu.roll(one, lane // 2, 1)),
                    jnp.where(low, pltpu.roll(two, lane // 2, 1), two),
                )
                return 0

            lax.fori_loop(0, blocks // 2, pair, 0)
            lend_copy(d).start()

    take_a(0).start()
    take_a(0).wait()
    split_a(0)
    lend(0)

    @pl.when(inner)
    def _():
        def early(j, _):
            relay(j)

            @pl.when(j + LEAD < chunks)
            def _():
                own_out(j + LEAD)

            return 0

        lax.fori_loop(0, min(AHEAD, chunks), early, 0)

    for d in range(1, classes):
        a_copy(d).wait_recv()
        take_a(d).start()
        if d > 1:
            take_a(d - 1).wait()
            split_a(d - 1)
            lend(d - 1)
    take_a(classes - 1).wait()
    split_a(classes - 1)
    lend(classes - 1)

    def order(p):
        return [(p + i) % levels for i in range(levels)]

    def place(p, d):
        at = 0
        for bit in order(p):
            at = 2 * at + (d // (1 << bit)) % 2
        return at

    def c_copy(j, p, level):
        count = classes >> (level + 1)
        peer = flip(c, 1 << order(p)[level], classes)
        return remote(
            cpart.at[j % slots, p, pl.ds(count, count)],
            rland.at[j, p, pl.ds(classes - 2 * count, count)],
            c_send.at[j, p, level], c_recv.at[j, p, level], (peer, s),
        )

    share = ncol // o_sem.shape[0]

    def out_copy(g):
        at = pl.ds(pl.multiple_of(g * share, share), share)
        return pltpu.make_async_copy(flat.at[:, at, :], o_ref.at[:, at, :], o_sem.at[g])

    late = -(-given * per // share)

    def back_copy(i):
        return remote(back.at[i], back.at[i], back_send.at[i], back_recv.at[i], friend)

    def reduce(j, level):
        count = classes >> (level + 1)
        held = j % slots
        for p in range(per):
            c_copy(j, p, level).wait_recv()
            if level + 1 < levels:
                cpart[held, p, 0:count] = (
                    cpart[held, p, 0:count] + rland[j, p, classes - 2 * count:classes - count]
                )
                c_copy(j, p, level + 1).start()
                continue

            @pl.when(j < chunks)
            def _():
                rows_of[pl.ds(j * per + p, rows, stride=ncol), :] = (
                    cpart[held, p, 0] + rland[j, p, classes - 2]
                )

            if given:
                @pl.when(j >= chunks)
                def _():
                    back[j - chunks, p] = cpart[held, p, 0] + rland[j, p, classes - 2]
        if level + 1 == levels:
            group = (j + 1) // (share // per) - 1

            @pl.when((j < chunks) & ((j + 1) % (share // per) == 0) & (inner | (group >= late)))
            def _():
                out_copy(group).start()

            if given:
                @pl.when(j >= chunks)
                def _():
                    back_copy(j - chunks).start()

    def gather(j, band):
        for owner in range(subs):
            @pl.when(owner // (subs // bands) == band)
            def _():
                @pl.when(s == owner)
                def _():
                    own_keep(j).wait()

                @pl.when((core != owner % 2) & (inner | (j >= given) | (spot == owner // 2)))
                def _():
                    at = slot(j, owner)
                    remote(at, at, peer_send.at[j, owner // 2], peer_recv.at[j, owner // 2], mate).wait_recv()

    def take_b(j, band, held):
        at = pl.ds(pl.multiple_of(band * lane, lane), lane)
        return pltpu.make_async_copy(ball.at[j, :, at, :], bstage.at[held], b_load.at[held])

    def split_b(held, size=lane, begin=0, step=lane):
        def split(g, _):
            value = bstage[held, g, 0:size, :]
            high = value.astype(jnp.bfloat16)
            at = pl.ds(pl.multiple_of(g * step + begin, size), size)
            bhi[at, :] = high
            blo[at, :] = (value - high.astype(jnp.float32)).astype(jnp.bfloat16)
            return 0

        lax.fori_loop(0, blocks, split, 0)

    part_rows = 2 * piece

    def take_part(j, held):
        at = pl.ds(pl.multiple_of(spot * part_rows, part_rows), part_rows)
        return pltpu.make_async_copy(
            ball.at[j, :, at, :], bstage.at[held, :, pl.ds(0, part_rows), :], b_load.at[held]
        )

    def clear_part(begin):
        def clear(g, _):
            at = pl.ds(pl.multiple_of(g * lane + begin, part_rows), part_rows)
            bhi[at, :] = jnp.zeros((part_rows, width), jnp.bfloat16)
            blo[at, :] = jnp.zeros((part_rows, width), jnp.bfloat16)
            return 0

        lax.fori_loop(0, blocks, clear, 0)

    def settle(j):
        for p in range(per):
            for level in range(levels):
                c_copy(j, p, level).wait_send()

    def multiply(j, left, deep, first):
        dot = functools.partial(jnp.dot, preferred_element_type=jnp.float32)
        held = j % slots

        def part(d, _):
            at = pl.ds(pl.multiple_of(d * rows, rows), rows)
            high, low = left(at)
            total = dot(high, bhi[0:deep]) + dot(high, blo[0:deep]) + dot(low, bhi[0:deep])
            for p in range(per):
                value = total[:, p * lane:(p + 1) * lane]
                to = place(p, d)
                cpart[held, p, to] = value if first else cpart[held, p, to] + value
            return 0

        lax.fori_loop(0, classes, part, 0)

    def mine(band):
        return lambda at: (ahi[band, at, :], alo[band, at, :])

    def theirs(begin, deep):
        return lambda at: (hhi[at, begin:begin + deep], hlo[at, begin:begin + deep])

    def sum_first(k, _):
        reduce(k, 0)
        return 0

    def sum_rest(k, _):
        for level in range(1, levels):
            reduce(k, level)
        return 0

    calm = jnp.where(outer, chunks * CALM // 16, chunks + given)

    def first_sums(j):
        return jnp.where(j > calm, j, jnp.maximum(j - 1, 0))

    def last_sums(j):
        return jnp.where(j > calm, j, jnp.maximum(j - 2, 0))

    def sums(body, begin, end):
        lax.fori_loop(begin, jnp.maximum(begin, end), body, 0)

    def step(j, _):
        @pl.when(inner)
        def _():
            relay(j + AHEAD)

            @pl.when(j + AHEAD + LEAD < chunks)
            def _():
                own_out(j + AHEAD + LEAD)

        @pl.when(outer)
        def _():
            forward(j, 1)

        alone = outer & (j < given)
        whole = inner | (j >= given)
        gather(j, near)

        @pl.when(whole)
        def _():
            take_b(j, near, 0).start()

        if given:
            @pl.when(alone)
            def _():
                take_part(j, 0).start()

        sums(sum_first, first_sums(j - 1), j - 1)

        @pl.when(j >= slots)
        def _():
            settle(j - slots)

        @pl.when(whole)
        def _():
            take_b(j, near, 0).wait()
            split_b(0)

        if given:
            @pl.when(alone)
            def _():
                take_part(j, 0).wait()
                split_b(0, part_rows, (spot % 2) * part_rows)
                clear_part((1 - spot % 2) * part_rows)

        multiply(j, mine(near), blocks * lane, True)
        sums(sum_first, jnp.maximum(j - 1, 0), first_sums(j))

        @pl.when(outer)
        def _():
            for dist in range(2, spots):
                forward(j, dist)

        sums(sum_rest, last_sums(j - 1), j - 2)

        @pl.when(whole)
        def _():
            for k in range(1, bands):
                band = (near + k) % bands
                gather(j, band)
                take_b(j, band, k % 2).start()
                take_b(j, band, k % 2).wait()
                split_b(k % 2)
                multiply(j, mine(band), blocks * lane, False)

        for p in range(per):
            c_copy(j, p, 0).start()
        sums(sum_rest, jnp.maximum(last_sums(j - 1), j - 2), last_sums(j))
        return 0

    lax.fori_loop(0, chunks, step, 0)

    def take_lent(d):
        lend_copy(d).wait_recv()

        def one(g, _):
            at = pl.ds(pl.multiple_of(g * lane, lane), lane)
            value = lent[d, :, at]
            high = value.astype(jnp.bfloat16)
            hhi[d * rows:(d + 1) * rows, at] = high
            hlo[d * rows:(d + 1) * rows, at] = (value - high.astype(jnp.float32)).astype(jnp.bfloat16)
            return 0

        lax.fori_loop(0, lent.shape[2] // lane, one, 0)

    def extra(i, _):
        j = chunks + i
        take_part(i, 0).start()
        sums(sum_first, first_sums(j - 1), first_sums(j))
        settle(j - slots)
        take_part(i, 0).wait()
        split_b(0, part_rows, 0, part_rows)
        multiply(j, theirs((bands - 1) * blocks * lane, blocks * part_rows), blocks * part_rows, True)
        for k in range(1, bands):
            take_b(i, (near + k) % bands, k % 2).start()
            if k == 1:
                sums(sum_rest, last_sums(j - 1), last_sums(j))
            take_b(i, (near + k) % bands, k % 2).wait()
            split_b(k % 2)
            multiply(j, theirs((k - 1) * blocks * lane, blocks * lane), blocks * lane, False)
        for p in range(per):
            c_copy(j, p, 0).start()
        return 0

    if given:
        @pl.when(helps)
        def _():
            for d in range(classes):
                take_lent(d)
            lax.fori_loop(0, given, extra, 0)

    def last(k, _):
        reduce(k, 0)

        @pl.when(k > last_sums(total - 1))
        def _():
            sum_rest(k - 1, 0)

        return 0

    lax.fori_loop(first_sums(total - 1), total, last, 0)
    sum_rest(total - 1, 0)

    if given:
        @pl.when(outer)
        def _():
            for i in range(given):
                back_copy(i).wait_recv()
                for p in range(per):
                    at = pl.ds(i * per + p, rows, stride=ncol)
                    rows_of[at, :] = rows_of[at, :] + back[i, p]
            for g in range(late):
                out_copy(g).start()

    for g in range(o_sem.shape[0]):
        out_copy(g).wait()

    def finish(j, _):
        own_mate(j).wait_send()
        for side in range(2):
            @pl.when(feeds(j, side))
            def _():
                own_line(j, side).wait_send()
            for dist in range(1, spots):
                @pl.when(gets(j, side, dist))
                def _():
                    @pl.when(feeds(j, side))
                    def _():
                        onward(j, side, dist).wait_send()
                    across(j, side, dist).wait_send()
        return 0

    lax.fori_loop(0, chunks, finish, 0)

    def settled(j, _):
        settle(j)
        return 0

    lax.fori_loop(total - slots, total, settled, 0)
    for d in range(1, classes):
        a_copy(d).wait_send()
    if given:
        @pl.when(outer)
        def _():
            for d in range(classes):
                lend_copy(d).wait_send()

        @pl.when(helps)
        def _():
            for i in range(given):
                back_copy(i).wait_send()


def streamed(classes, subs, first_factor_tiles, b_blocks):
    blocks, q, halves, cols, order = first_factor_tiles.shape
    wide = b_blocks.shape[4]
    lane, sub = LANE, SUBLANE
    rows, bands, ncol = blocks * q, order // (LANE * classes), halves * cols * wide // LANE
    left = first_factor_tiles.reshape(rows, halves, cols, classes * bands, lane)
    left = jnp.transpose(left, (0, 1, 3, 2, 4)).reshape(rows * halves, classes, bands * cols, lane)
    right = b_blocks.reshape(rows, halves, cols, wide // lane, lane)
    right = jnp.transpose(right, (0, 1, 3, 2, 4)).reshape(rows, ncol, lane)
    lead, unit = rows * halves, bands * cols
    per = 2
    chunks, width, depth = ncol // per, per * lane, bands * lane
    dma = pltpu.SemaphoreType.DMA
    f32, bf16 = jnp.float32, jnp.bfloat16
    spots, levels = subs // 2, classes.bit_length() - 1
    given = chunks * GIVEN // 16 if spots > 3 and spots == 2 * bands and blocks % 2 == 0 else 0
    deep = (2 * bands - 1) * blocks * lane // 2
    some = max(given, 1)
    out, _, _ = pl.pallas_call(
        functools.partial(stream, classes, subs, given),
        out_shape=(
            jax.ShapeDtypeStruct((rows, ncol, lane), f32),
            jax.ShapeDtypeStruct((classes - 1, lead, unit, lane), f32),
            jax.ShapeDtypeStruct((chunks, blocks, depth, width), f32),
        ),
        in_specs=[pl.BlockSpec(memory_space=pl.ANY)] * 2,
        out_specs=(pl.BlockSpec(memory_space=pl.ANY),) * 3,
        scratch_shapes=[
            pltpu.VMEM((rows, ncol, lane), f32),
            pltpu.VMEM((chunks, blocks, q, width), f32),
            pltpu.VMEM((2, lead, unit, lane), f32),
            pltpu.VMEM((bands, classes * rows, blocks * lane), bf16),
            pltpu.VMEM((bands, classes * rows, blocks * lane), bf16),
            pltpu.VMEM((2, blocks, lane, width), f32),
            pltpu.VMEM((blocks * lane, width), bf16),
            pltpu.VMEM((blocks * lane, width), bf16),
            pltpu.VMEM((min(SLOTS, chunks), per, classes, rows, lane), f32),
            pltpu.VMEM((chunks + given, per, classes - 1, rows, lane), f32),
            pltpu.VMEM((classes, rows, deep), f32),
            pltpu.VMEM((classes * rows, deep), bf16),
            pltpu.VMEM((classes * rows, deep), bf16),
            pltpu.VMEM((some, per, rows, lane), f32),
            dma((classes,)),
            dma((classes,)),
            dma((classes,)),
            dma((classes,)),
            dma((some,)),
            dma((some,)),
            dma((2, chunks)),
            dma((2, chunks, spots)),
            dma((2, chunks, spots)),
            dma((chunks, spots)),
            dma((chunks, spots)),
            dma((chunks,)),
            dma((chunks + given, per, levels)),
            dma((chunks + given, per, levels)),
            dma((2,)),
            dma((2,)),
            dma((ncol // sub,)),
        ],
        compiler_params=pltpu.CompilerParams(
            collective_id=0, has_side_effects=True, vmem_limit_bytes=62 * 1024 * 1024
        ),
    )(left, right)
    out = out.reshape(rows, halves, wide // lane, cols, lane)
    return jnp.transpose(out, (0, 1, 3, 2, 4)).reshape(b_blocks.shape)


def fits(classes, subs, first_factor_tiles, b_blocks):
    blocks, q, halves, cols, order = first_factor_tiles.shape
    bands, spots = order // (LANE * classes), subs // 2
    return (
        classes > 1 and bands > 1 and q % SUBLANE == 0 and order % (LANE * classes) == 0 and (bands * cols) % SUBLANE == 0
        and bands * LANE == subs * q and spots % bands == 0
    )


def either(classes, subs, first_factor_tiles, b_blocks):
    pick = streamed if fits(classes, subs, first_factor_tiles, b_blocks) else local
    return pick(classes, subs, first_factor_tiles, b_blocks)


def solution(mesh):
    spec = P(None, ("cls", "str"), None, None, None)
    return jax.shard_map(
        functools.partial(either, mesh.shape["cls"], mesh.shape["str"]),
        mesh=mesh, in_specs=(spec, spec), out_specs=spec, check_vma=False,
    )
```

```python
import functools

import jax
import jax.numpy as jnp
from jax import lax
from jax.experimental import pallas as pl
from jax.experimental.pallas import tpu as pltpu
from jax.sharding import PartitionSpec as P

MESH = pl.DeviceIdType.MESH
LAG = 3
EARLY = 2
AHEAD = 7
OUTER = 3
EARLY_RELAYS = ((3, 2), (5, 3), (7, 5))
TURN = 1
LEAD = 2
MORE = 2
GIVEN = 2
SLOTS = 8
CALM = 14
LANE = 128
SUBLANE = 8


def flip(index, mask, count):
    out, bit = index, 1
    while bit < count:
        have, want = (index // bit) % 2, (mask // bit) % 2
        out = out + want * (1 - 2 * have) * bit
        bit *= 2
    return out


def kernel(
    classes, subs, a_ref, b_ref, o_ref, aland, ball,
    ahi, alo, astage, bstage, bhi, blo, cpart, rland,
    a_send, a_recv, own_send, fwd_send, line_recv, peer_send, peer_recv,
    c_send, c_recv, a_load, b_load, o_sem,
):
    chunks, groups, piece, width = b_ref.shape
    rows = a_ref.shape[1]
    depth = subs * piece
    spots = subs // 2
    c, s = lax.axis_index("cls"), lax.axis_index("str")
    spot, core = s // 2, s % 2
    mate = (c, s + 1 - 2 * core)
    beside = ((c, s - 2), (c, s + 2))
    has = (spot > 0, spot < spots - 1)

    barrier = pltpu.get_barrier_semaphore()
    for d in range(1, classes):
        pl.semaphore_signal(barrier, inc=1, device_id=(flip(c, d, classes), s), device_id_type=MESH)
    pl.semaphore_signal(barrier, inc=1, device_id=mate, device_id_type=MESH)
    for side in range(2):
        @pl.when(has[side])
        def _():
            pl.semaphore_signal(barrier, inc=1, device_id=beside[side], device_id_type=MESH)
    lower, higher = (spot + spots - 1) // spots, (2 * spots - 2 - spot) // spots
    pl.semaphore_wait(barrier, classes + lower + higher)

    def remote(src, dst, send, recv, to):
        return pltpu.make_async_remote_copy(
            src_ref=src, dst_ref=dst, send_sem=send, recv_sem=recv,
            device_id=to, device_id_type=MESH,
        )

    def slot(j, owner):
        return ball.at[j, :, pl.ds(pl.multiple_of(owner * piece, piece), piece), :]

    def own_line(j, side):
        return remote(b_ref.at[j], slot(j, s), own_send.at[side, j], line_recv.at[side, j, 0], beside[side])

    def own_mate(j):
        return remote(b_ref.at[j], slot(j, s), peer_send.at[j, spot], peer_recv.at[j, spot], mate)

    def origin(side, dist):
        return spot + dist if side == 0 else spot - dist

    def there(side, dist):
        return spot + dist < spots if side == 0 else spot >= dist

    def arrival(j, side, dist):
        at = slot(j, 2 * origin(side, dist) + core)
        return remote(at, at, own_send.at[side, j], line_recv.at[side, j, dist - 1], beside[1 - side])

    def onward(j, side, dist):
        at = slot(j, 2 * origin(side, dist) + core)
        return remote(at, at, fwd_send.at[side, j, dist - 1], line_recv.at[side, j, dist], beside[side])

    def across(j, side, dist):
        begin = origin(side, dist)
        at = slot(j, 2 * begin + core)
        return remote(at, at, peer_send.at[j, begin], peer_recv.at[j, begin], mate)

    def forward(j, dist):
        for side in range(2):
            @pl.when(there(side, dist))
            def _():
                arrival(j, side, dist).wait_recv()

                @pl.when(has[side])
                def _():
                    onward(j, side, dist).start()

                across(j, side, dist).start()

    def a_copy(d):
        peer = flip(c, d, classes)
        return remote(
            a_ref.at[:, :, pl.ds(pl.multiple_of(peer * depth, depth), depth)],
            aland.at[:, pl.ds(pl.multiple_of(c * rows, rows), rows), :],
            a_send.at[d], a_recv.at[d], (peer, s),
        )

    for d in range(1, classes):
        a_copy(d).start()

    def begin(j, _):
        for side in range(2):
            @pl.when(has[side])
            def _():
                own_line(j, side).start()
        own_mate(j).start()
        return 0

    lax.fori_loop(0, chunks, begin, 0)

    for j in range(min(EARLY, chunks)):
        forward(j, 1)
    for d in range(1, classes):
        a_copy(d).wait_recv()

    def load_a(g, held):
        for e in range(classes):
            to = astage.at[held, pl.ds(e * rows, rows), :]

            @pl.when(c == e)
            def _():
                pltpu.make_async_copy(
                    a_ref.at[g, :, pl.ds(pl.multiple_of(c * depth, depth), depth)], to, a_load.at[held]
                ).start()

            @pl.when(c != e)
            def _():
                pltpu.make_async_copy(aland.at[g, pl.ds(e * rows, rows), :], to, a_load.at[held]).start()

    load_a(0, 0)
    for g in range(groups):
        held = g % 2
        if g + 1 < groups:
            load_a(g + 1, 1 - held)
        pltpu.make_async_copy(aland.at[g], astage.at[held], a_load.at[held]).wait()

        def split(m, _, held=held, g=g):
            at = pl.ds(pl.multiple_of(m * rows, rows), rows)
            value = astage[held, at, :]
            high = value.astype(jnp.bfloat16)
            ahi[at, g * depth:(g + 1) * depth] = high
            alo[at, g * depth:(g + 1) * depth] = (value - high.astype(jnp.float32)).astype(jnp.bfloat16)
            return 0

        lax.fori_loop(0, classes, split, 0)

    def c_copy(j, d):
        peer = flip(c, d, classes)
        return remote(
            cpart.at[j, pl.ds(pl.multiple_of(peer * rows, rows), rows), :],
            rland.at[j, d - 1], c_send.at[j, d], c_recv.at[j, d], (peer, s),
        )

    mine = pl.ds(pl.multiple_of(c * rows, rows), rows)

    def out_copy(j):
        return pltpu.make_async_copy(cpart.at[j, mine, :], o_ref.at[j], o_sem.at[j])

    def reduce(j):
        for d in range(1, classes):
            c_copy(j, d).wait_recv()
        total = cpart[j, mine, :]
        for d in range(1, classes):
            total = total + rland[j, d - 1]
        cpart[j, mine, :] = total
        out_copy(j).start()

    def step(j, _):
        if spots > 1:
            @pl.when(j + EARLY < chunks)
            def _():
                forward(j + EARLY, 1)
        for dist in range(2, spots):
            forward(j, dist)

        for owner in range(subs):
            to = bstage.at[:, pl.ds(owner * piece, piece), :]

            @pl.when(s == owner)
            def _():
                pltpu.make_async_copy(b_ref.at[j], to, b_load.at[0]).start()

            @pl.when(s != owner)
            def _():
                @pl.when(core != owner % 2)
                def _():
                    remote(to_slot(j, owner), to_slot(j, owner), peer_send.at[j, owner // 2],
                           peer_recv.at[j, owner // 2], mate).wait_recv()

                pltpu.make_async_copy(to_slot(j, owner), to, b_load.at[0]).start()

        pltpu.make_async_copy(ball.at[j], bstage, b_load.at[0]).wait()

        def split(g, _):
            value = bstage[g]
            high = value.astype(jnp.bfloat16)
            at = pl.ds(pl.multiple_of(g * depth, depth), depth)
            bhi[at, :] = high
            blo[at, :] = (value - high.astype(jnp.float32)).astype(jnp.bfloat16)
            return 0

        lax.fori_loop(0, groups, split, 0)

        def part(i, _):
            d = (i + 1) % classes
            at = pl.ds(pl.multiple_of(flip(c, d, classes) * rows, rows), rows)
            dot = functools.partial(jnp.dot, preferred_element_type=jnp.float32)
            cpart[j, at, :] = (
                dot(ahi[at, :], bhi[...]) + dot(ahi[at, :], blo[...]) + dot(alo[at, :], bhi[...])
            )

            @pl.when(d != 0)
            def _():
                c_copy(j, d).start()

            return 0

        lax.fori_loop(0, classes, part, 0)

        @pl.when(j >= LAG)
        def _():
            reduce(j - LAG)

        return 0

    def to_slot(j, owner):
        return ball.at[j, :, pl.ds(owner * piece, piece), :]

    lax.fori_loop(0, chunks, step, 0)
    for j in range(max(chunks - LAG, 0), chunks):
        reduce(j)

    def finish(j, _):
        out_copy(j).wait()
        own_mate(j).wait_send()
        for d in range(1, classes):
            c_copy(j, d).wait_send()
        for side in range(2):
            @pl.when(has[side])
            def _():
                own_line(j, side).wait_send()
            for dist in range(1, spots):
                @pl.when(there(side, dist))
                def _():
                    @pl.when(has[side])
                    def _():
                        onward(j, side, dist).wait_send()
                    across(j, side, dist).wait_send()
        return 0

    lax.fori_loop(0, chunks, finish, 0)
    for d in range(1, classes):
        a_copy(d).wait_send()


def local(classes, subs, first_factor_tiles, b_blocks):
    blocks, q, halves, cols, order = first_factor_tiles.shape
    inner, width = halves * cols, b_blocks.shape[4]
    rows = blocks * q
    left = first_factor_tiles.reshape(rows, inner, order)
    right = jnp.transpose(b_blocks.reshape(inner, q, inner, width), (2, 0, 1, 3))
    if q % 8 == 0:
        left = jnp.transpose(left, (1, 0, 2))
    else:
        left = left.reshape(rows, inner, classes * subs, q)
        left = jnp.transpose(left, (0, 2, 1, 3)).reshape(1, rows, inner * order)
        right = right.reshape(inner, 1, inner * q, width)
    chunks, groups, piece, _ = right.shape
    depth = subs * piece
    dma = pltpu.SemaphoreType.DMA
    f32, bf16 = jnp.float32, jnp.bfloat16
    spots = subs // 2
    out, _, _ = pl.pallas_call(
        functools.partial(kernel, classes, subs),
        out_shape=(
            jax.ShapeDtypeStruct((chunks, rows, width), f32),
            jax.ShapeDtypeStruct((groups, classes * rows, depth), f32),
            jax.ShapeDtypeStruct((chunks, groups, depth, width), f32),
        ),
        in_specs=[pl.BlockSpec(memory_space=pl.ANY)] * 2,
        out_specs=(pl.BlockSpec(memory_space=pl.ANY),) * 3,
        scratch_shapes=[
            pltpu.VMEM((classes * rows, groups * depth), bf16),
            pltpu.VMEM((classes * rows, groups * depth), bf16),
            pltpu.VMEM((2, classes * rows, depth), f32),
            pltpu.VMEM((groups, depth, width), f32),
            pltpu.VMEM((groups * depth, width), bf16),
            pltpu.VMEM((groups * depth, width), bf16),
            pltpu.VMEM((chunks, classes * rows, width), f32),
            pltpu.VMEM((chunks, classes - 1, rows, width), f32),
            dma((classes,)),
            dma((classes,)),
            dma((2, chunks)),
            dma((2, chunks, spots)),
            dma((2, chunks, spots)),
            dma((chunks, spots)),
            dma((chunks, spots)),
            dma((chunks, classes)),
            dma((chunks, classes)),
            dma((2,)),
            dma((1,)),
            dma((chunks,)),
        ],
        compiler_params=pltpu.CompilerParams(
            collective_id=0, has_side_effects=True, vmem_limit_bytes=60 * 1024 * 1024
        ),
    )(left, right)
    out = jnp.transpose(out, (1, 0, 2))
    return out.reshape(b_blocks.shape)


def stream(
    classes, subs, given, a_ref, b_ref, o_ref, aland, ball,
    flat, bown, astage, ahi, alo, bstage, bhi, blo, cpart, rland, lent, hhi, hlo, back,
    a_send, a_recv, lend_send, lend_recv, back_send, back_recv, own_send, fwd_send, line_recv, peer_send, peer_recv, keep_sem,
    c_send, c_recv, a_load, b_load, o_sem,
):
    lead, _, unit, lane = a_ref.shape
    rows, ncol, _ = b_ref.shape
    chunks, blocks, depth, width = ball.shape
    bands = depth // lane
    piece = depth // subs
    per = width // lane
    levels = classes.bit_length() - 1
    spots = subs // 2
    c, s = lax.axis_index("cls"), lax.axis_index("str")
    spot, core = s // 2, s % 2
    mate = (c, s + 1 - 2 * core)
    beside = ((c, s - 2), (c, s + 2))
    has = (spot > 0, spot < spots - 1)
    inner = (spot > 0) & (spot < spots - 1)
    outer = (spot == 0) | (spot == spots - 1)
    near = spot // (spots // bands)
    slots = cpart.shape[0]
    helps = (spot == 1) | (spot == spots - 2)
    total = jnp.where(helps, chunks + given, chunks)
    ends = (spot == 1, spot == spots - 2)
    friend = (c, jnp.where((spot == 0) | (spot == spots - 2), s + 2, s - 2))

    barrier = pltpu.get_barrier_semaphore()
    for d in range(1, classes):
        pl.semaphore_signal(barrier, inc=1, device_id=(flip(c, d, classes), s), device_id_type=MESH)
    pl.semaphore_signal(barrier, inc=1, device_id=mate, device_id_type=MESH)
    for side in range(2):
        @pl.when(has[side])
        def _():
            pl.semaphore_signal(barrier, inc=1, device_id=beside[side], device_id_type=MESH)
    b_in = pltpu.make_async_copy(b_ref, flat, b_load.at[0])
    b_in.start()
    lower, higher = (spot + spots - 1) // spots, (2 * spots - 2 - spot) // spots
    pl.semaphore_wait(barrier, classes + lower + higher)

    def remote(src, dst, send, recv, to):
        return pltpu.make_async_remote_copy(
            src_ref=src, dst_ref=dst, send_sem=send, recv_sem=recv,
            device_id=to, device_id_type=MESH,
        )

    def a_copy(d):
        peer = flip(c, d, classes)
        return remote(a_ref.at[:, peer], aland.at[d - 1], a_send.at[d], a_recv.at[d], (peer, s))

    for d in range(1, classes):
        a_copy(d).start()

    def slot(j, owner):
        return ball.at[j, :, pl.ds(pl.multiple_of(owner * piece, piece), piece), :]

    def own_line(j, side):
        return remote(bown.at[j], slot(j, s), own_send.at[side, j], line_recv.at[side, j, 0], beside[side])

    def own_mate(j):
        return remote(bown.at[j], slot(j, s), peer_send.at[j, spot], peer_recv.at[j, spot], mate)

    def own_keep(j):
        return pltpu.make_async_copy(bown.at[j], slot(j, s), keep_sem.at[j])

    def origin(side, dist):
        return spot + dist if side == 0 else spot - dist

    def there(side, dist):
        return spot + dist < spots if side == 0 else spot >= dist

    def arrival(j, side, dist):
        at = slot(j, 2 * origin(side, dist) + core)
        return remote(at, at, own_send.at[side, j], line_recv.at[side, j, dist - 1], beside[1 - side])

    def onward(j, side, dist):
        at = slot(j, 2 * origin(side, dist) + core)
        return remote(at, at, fwd_send.at[side, j, dist - 1], line_recv.at[side, j, dist], beside[side])

    def across(j, side, dist):
        begin = origin(side, dist)
        at = slot(j, 2 * begin + core)
        return remote(at, at, peer_send.at[j, begin], peer_recv.at[j, begin], mate)

    def forward(j, dist):
        for side in range(2):
            @pl.when(gets(j, side, dist))
            def _():
                arrival(j, side, dist).wait_recv()

                @pl.when(feeds(j, side))
                def _():
                    onward(j, side, dist).start()

                across(j, side, dist).start()

    def relay(t, _):
        for dist in range(1, spots):
            at = jnp.where(inner, t - dist + 1, t)

            @pl.when((at >= 0) & (at < chunks))
            def _():
                forward(at, dist)

        @pl.when(inner & (t + LEAD < chunks))
        def _():
            own_out(t + LEAD)

        return 0

    def ready(t):
        slow = jnp.maximum(t + 1, given + OUTER + (t + 1) // 2)
        fast = AHEAD + 1 + (3 * t) // 4
        return jnp.minimum(jnp.where(inner, jnp.maximum(fast, t + spots), slow), chunks + spots - 2)

    def feeds(j, side):
        return has[side] & ((j >= given) | jnp.logical_not(ends[side]))

    def gets(j, side, dist):
        return there(side, dist) & ((j >= given) | inner)

    shift = given + MORE

    def own_out(j):
        for side in range(2):
            @pl.when(has[side] & jnp.logical_not(ends[side]))
            def _():
                own_line(j, side).start()

            @pl.when(ends[side] & (j + shift < chunks))
            def _():
                own_line(j + shift, side).start()

    b_in.wait()
    rows_of = flat.reshape(rows * ncol, lane)

    def lay(j):
        for p in range(per):
            value = rows_of[pl.ds(j * per + p, rows, stride=ncol), :]
            bown[j, :, :, p * lane:(p + 1) * lane] = value.reshape(blocks, piece, lane)

    first = min(LEAD + shift, chunks)
    for j in range(first):
        lay(j)
    for side in range(2):
        for j in range(given, min(given + MORE, chunks)):
            @pl.when(ends[side])
            def _():
                own_line(j, side).start()
    for j in range(min(LEAD, chunks)):
        own_out(j)

    def lay_more(j, _):
        lay(j)
        return 0

    lax.fori_loop(first, chunks, lay_more, 0)

    def begin(j, _):
        own_mate(j).start()
        own_keep(j).start()

        @pl.when(outer & (j >= LEAD))
        def _():
            own_out(j)

        return 0

    lax.fori_loop(0, chunks, begin, 0)

    def take_a(d):
        held = astage.at[d % 2]
        if d == 0:
            return pltpu.make_async_copy(a_ref.at[:, c], held, a_load.at[0])
        return pltpu.make_async_copy(aland.at[d - 1], held, a_load.at[d % 2])

    def split_a(d):
        lines = astage.at[d % 2].reshape(lead * unit, lane)
        stride = lead * unit // rows
        cols = unit // bands

        def one(k, _):
            h, band, col = k // unit, (k % unit) // cols, k % cols
            value = lines[pl.ds(k, rows, stride=stride), :]
            high = value.astype(jnp.bfloat16)
            at = pl.ds(pl.multiple_of((h * cols + col) * lane, lane), lane)
            ahi[band, d * rows:(d + 1) * rows, at] = high
            alo[band, d * rows:(d + 1) * rows, at] = (value - high.astype(jnp.float32)).astype(jnp.bfloat16)
            return 0

        lax.fori_loop(0, stride, one, 0)

    def lend_copy(d):
        return remote(lent.at[d], lent.at[d], lend_send.at[d], lend_recv.at[d], friend)

    def lend(d):
        if not given:
            return
        lines = astage.at[d % 2].reshape(lead * unit, lane)
        stride = lead * unit // rows
        cols = unit // bands
        left = lax.broadcasted_iota(jnp.int32, (rows, lane), 1) < lane // 2
        low = spot % 2 == 1

        def block(g, band):
            return lines[pl.ds((g // cols) * unit + band * cols + g % cols, rows, stride=stride), :]

        @pl.when(outer)
        def _():
            for k in range(1, bands):
                def whole(g, _, k=k):
                    at = pl.ds(pl.multiple_of(((k - 1) * blocks + g) * lane, lane), lane)
                    lent[d, :, at] = block(g, (near + k) % bands)
                    return 0

                lax.fori_loop(0, blocks, whole, 0)

            def pair(g, _):
                one, two = block(2 * g, near), block(2 * g + 1, near)
                at = pl.ds(pl.multiple_of(((bands - 1) * blocks + g) * lane, lane), lane)
                lent[d, :, at] = jnp.where(
                    left,
                    jnp.where(low, one, pltpu.roll(one, lane // 2, 1)),
                    jnp.where(low, pltpu.roll(two, lane // 2, 1), two),
                )
                return 0

            lax.fori_loop(0, blocks // 2, pair, 0)
            lend_copy(d).start()

    take_a(0).start()
    take_a(0).wait()
    split_a(0)
    lend(0)

    def accept(d):
        a_copy(d).wait_recv()
        take_a(d).start()
        take_a(d).wait()
        split_a(d)
        lend(d)

    at = [jnp.where(inner, x, y) for x, y in EARLY_RELAYS]
    stops = [0] + [jnp.minimum(x, ready(-1)) for x in at]
    for d in range(1, classes):
        if d <= len(at):
            lax.fori_loop(stops[d - 1], stops[d], relay, 0)
        accept(d)
    lax.fori_loop(stops[min(len(at), classes - 1)], ready(-1), relay, 0)

    def order(p):
        return [(p + i) % levels for i in range(levels)]

    def place(p, d):
        at = 0
        for bit in order(p):
            at = 2 * at + (d // (1 << bit)) % 2
        return at

    def c_copy(j, p, level):
        count = classes >> (level + 1)
        peer = flip(c, 1 << order(p)[level], classes)
        return remote(
            cpart.at[j % slots, p, pl.ds(count, count)],
            rland.at[j, p, pl.ds(classes - 2 * count, count)],
            c_send.at[j, p, level], c_recv.at[j, p, level], (peer, s),
        )

    share = ncol // o_sem.shape[0]

    def out_copy(g):
        at = pl.ds(pl.multiple_of(g * share, share), share)
        return pltpu.make_async_copy(flat.at[:, at, :], o_ref.at[:, at, :], o_sem.at[g])

    turn = jnp.where(helps, chunks - TURN, chunks)

    def chunk_of(t):
        return jnp.where(helps & (t >= turn + given), t - given, t)

    def lent_at(t):
        return helps & (t >= turn) & (t < turn + given)

    late = -(-given * per // share)

    def back_copy(i):
        return remote(back.at[i], back.at[i], back_send.at[i], back_recv.at[i], friend)

    def reduce(j, level):
        count = classes >> (level + 1)
        held = j % slots
        for p in range(per):
            c_copy(j, p, level).wait_recv()
            if level + 1 < levels:
                cpart[held, p, 0:count] = (
                    cpart[held, p, 0:count] + rland[j, p, classes - 2 * count:classes - count]
                )
                c_copy(j, p, level + 1).start()
                continue

            @pl.when(jnp.logical_not(lent_at(j)))
            def _():
                rows_of[pl.ds(chunk_of(j) * per + p, rows, stride=ncol), :] = (
                    cpart[held, p, 0] + rland[j, p, classes - 2]
                )

            if given:
                @pl.when(lent_at(j))
                def _():
                    back[j - turn, p] = cpart[held, p, 0] + rland[j, p, classes - 2]
        if level + 1 == levels:
            count, done = share // per, chunk_of(j) + 1
            group = done // count - 1

            @pl.when(jnp.logical_not(lent_at(j)) & (done % count == 0) & (inner | (group >= late)))
            def _():
                out_copy(group).start()

            if given:
                @pl.when(lent_at(j))
                def _():
                    back_copy(j - turn).start()

    def gather(j, band):
        for owner in range(subs):
            @pl.when(owner // (subs // bands) == band)
            def _():
                @pl.when(s == owner)
                def _():
                    own_keep(j).wait()

                @pl.when((core != owner % 2) & (inner | (j >= given) | (spot == owner // 2)))
                def _():
                    at = slot(j, owner)
                    remote(at, at, peer_send.at[j, owner // 2], peer_recv.at[j, owner // 2], mate).wait_recv()

    def take_b(j, band, held):
        at = pl.ds(pl.multiple_of(band * lane, lane), lane)
        return pltpu.make_async_copy(ball.at[j, :, at, :], bstage.at[held], b_load.at[held])

    def split_b(held, size=lane, begin=0, step=lane):
        def split(g, _):
            value = bstage[held, g, 0:size, :]
            high = value.astype(jnp.bfloat16)
            at = pl.ds(pl.multiple_of(g * step + begin, size), size)
            bhi[at, :] = high
            blo[at, :] = (value - high.astype(jnp.float32)).astype(jnp.bfloat16)
            return 0

        lax.fori_loop(0, blocks, split, 0)

    part_rows = 2 * piece

    def take_part(j, held):
        at = pl.ds(pl.multiple_of(spot * part_rows, part_rows), part_rows)
        return pltpu.make_async_copy(
            ball.at[j, :, at, :], bstage.at[held, :, pl.ds(0, part_rows), :], b_load.at[held]
        )

    def clear_part(begin):
        def clear(g, _):
            at = pl.ds(pl.multiple_of(g * lane + begin, part_rows), part_rows)
            bhi[at, :] = jnp.zeros((part_rows, width), jnp.bfloat16)
            blo[at, :] = jnp.zeros((part_rows, width), jnp.bfloat16)
            return 0

        lax.fori_loop(0, blocks, clear, 0)

    def settle(j):
        for p in range(per):
            for level in range(levels):
                c_copy(j, p, level).wait_send()

    def multiply(j, left, deep, first):
        dot = functools.partial(jnp.dot, preferred_element_type=jnp.float32)
        held = j % slots

        def part(d, _):
            at = pl.ds(pl.multiple_of(d * rows, rows), rows)
            high, low = left(at)
            total = dot(high, bhi[0:deep]) + dot(high, blo[0:deep]) + dot(low, bhi[0:deep])
            for p in range(per):
                value = total[:, p * lane:(p + 1) * lane]
                to = place(p, d)
                cpart[held, p, to] = value if first else cpart[held, p, to] + value
            return 0

        lax.fori_loop(0, classes, part, 0)

    def mine(band):
        return lambda at: (ahi[band, at, :], alo[band, at, :])

    def theirs(begin, deep):
        return lambda at: (hhi[at, begin:begin + deep], hlo[at, begin:begin + deep])

    def sum_first(k, _):
        reduce(k, 0)
        return 0

    def sum_rest(k, _):
        for level in range(1, levels):
            reduce(k, level)
        return 0

    calm = jnp.where(outer, chunks * CALM // 16, chunks + given)

    def first_sums(j):
        return jnp.where(j > calm, j, jnp.maximum(j - 1, 0))

    def last_sums(j):
        return jnp.where(j > calm, j, jnp.maximum(j - 2, 0))

    def sums(body, begin, end):
        lax.fori_loop(begin, jnp.maximum(begin, end), body, 0)

    def usual(t):
        j = chunk_of(t)
        lax.fori_loop(ready(j - 1), ready(j), relay, 0)
        alone = outer & (j < given)
        whole = inner | (j >= given)
        gather(j, near)

        @pl.when(whole)
        def _():
            take_b(j, near, 0).start()

        @pl.when(inner)
        def _():
            gather(j, (near + 1) % bands)
            take_b(j, (near + 1) % bands, 1).start()

        if given:
            @pl.when(alone)
            def _():
                take_part(j, 0).start()

        sums(sum_first, first_sums(t - 1), t - 1)

        @pl.when(t >= slots)
        def _():
            settle(t - slots)

        @pl.when(whole)
        def _():
            take_b(j, near, 0).wait()
            split_b(0)

        if given:
            @pl.when(alone)
            def _():
                take_part(j, 0).wait()
                split_b(0, part_rows, (spot % 2) * part_rows)
                clear_part((1 - spot % 2) * part_rows)

        multiply(t, mine(near), blocks * lane, True)
        sums(sum_first, jnp.maximum(t - 1, 0), first_sums(t))

        @pl.when(whole)
        def _():
            for k in range(1, bands):
                band = (near + k) % bands

                @pl.when(outer | (k > 1))
                def _():
                    gather(j, band)
                    take_b(j, band, k % 2).start()

                if k == 1:
                    sums(sum_rest, last_sums(t - 1), t - 2)
                take_b(j, band, k % 2).wait()
                split_b(k % 2)
                multiply(t, mine(band), blocks * lane, False)

        @pl.when(alone)
        def _():
            sums(sum_rest, last_sums(t - 1), t - 2)

    def take_lent(d):
        lend_copy(d).wait_recv()

        def one(g, _):
            at = pl.ds(pl.multiple_of(g * lane, lane), lane)
            value = lent[d, :, at]
            high = value.astype(jnp.bfloat16)
            hhi[d * rows:(d + 1) * rows, at] = high
            hlo[d * rows:(d + 1) * rows, at] = (value - high.astype(jnp.float32)).astype(jnp.bfloat16)
            return 0

        lax.fori_loop(0, lent.shape[2] // lane, one, 0)

    def extra(t):
        i = t - turn
        take_part(i, 0).start()
        for k in range(1, bands):
            if k == 1:
                take_b(i, (near + k) % bands, k % 2).start()
        sums(sum_first, first_sums(t - 1), first_sums(t))

        @pl.when(t >= slots)
        def _():
            settle(t - slots)

        @pl.when(i == 0)
        def _():
            for d in range(classes):
                take_lent(d)

        take_part(i, 0).wait()
        split_b(0, part_rows, 0, part_rows)
        multiply(t, theirs((bands - 1) * blocks * lane, blocks * part_rows), blocks * part_rows, True)
        for k in range(1, bands):
            if k > 1:
                take_b(i, (near + k) % bands, k % 2).start()
            if k == 1:
                sums(sum_rest, last_sums(t - 1), last_sums(t))
            take_b(i, (near + k) % bands, k % 2).wait()
            split_b(k % 2)
            multiply(t, theirs((k - 1) * blocks * lane, blocks * lane), blocks * lane, False)

    def step(t, _):
        if given:
            @pl.when(lent_at(t))
            def _():
                extra(t)

        @pl.when(jnp.logical_not(lent_at(t)))
        def _():
            usual(t)

        for p in range(per):
            c_copy(t, p, 0).start()
        sums(sum_rest, jnp.maximum(last_sums(t - 1), t - 2), last_sums(t))
        return 0

    lax.fori_loop(0, total, step, 0)

    def last(k, _):
        reduce(k, 0)

        @pl.when(k > last_sums(total - 1))
        def _():
            sum_rest(k - 1, 0)

        return 0

    lax.fori_loop(first_sums(total - 1), total, last, 0)
    sum_rest(total - 1, 0)

    if given:
        @pl.when(outer)
        def _():
            for i in range(given):
                back_copy(i).wait_recv()
                for p in range(per):
                    at = pl.ds(i * per + p, rows, stride=ncol)
                    rows_of[at, :] = rows_of[at, :] + back[i, p]
            for g in range(late):
                out_copy(g).start()

    for g in range(o_sem.shape[0]):
        out_copy(g).wait()

    def finish(j, _):
        own_mate(j).wait_send()
        for side in range(2):
            @pl.when(feeds(j, side))
            def _():
                own_line(j, side).wait_send()
            for dist in range(1, spots):
                @pl.when(gets(j, side, dist))
                def _():
                    @pl.when(feeds(j, side))
                    def _():
                        onward(j, side, dist).wait_send()
                    across(j, side, dist).wait_send()
        return 0

    lax.fori_loop(0, chunks, finish, 0)

    def settled(j, _):
        settle(j)
        return 0

    lax.fori_loop(total - slots, total, settled, 0)
    for d in range(1, classes):
        a_copy(d).wait_send()
    if given:
        @pl.when(outer)
        def _():
            for d in range(classes):
                lend_copy(d).wait_send()

        @pl.when(helps)
        def _():
            for i in range(given):
                back_copy(i).wait_send()


def streamed(classes, subs, first_factor_tiles, b_blocks):
    blocks, q, halves, cols, order = first_factor_tiles.shape
    wide = b_blocks.shape[4]
    lane, sub = LANE, SUBLANE
    rows, bands, ncol = blocks * q, order // (LANE * classes), halves * cols * wide // LANE
    left = first_factor_tiles.reshape(rows, halves, cols, classes * bands, lane)
    left = jnp.transpose(left, (0, 1, 3, 2, 4)).reshape(rows * halves, classes, bands * cols, lane)
    right = b_blocks.reshape(rows, halves, cols, wide // lane, lane)
    right = jnp.transpose(right, (0, 1, 3, 2, 4)).reshape(rows, ncol, lane)
    lead, unit = rows * halves, bands * cols
    per = 2
    chunks, width, depth = ncol // per, per * lane, bands * lane
    dma = pltpu.SemaphoreType.DMA
    f32, bf16 = jnp.float32, jnp.bfloat16
    spots, levels = subs // 2, classes.bit_length() - 1
    given = chunks * GIVEN // 16 if spots > 3 and spots == 2 * bands and blocks % 2 == 0 else 0
    deep = (2 * bands - 1) * blocks * lane // 2
    some = max(given, 1)
    out, _, _ = pl.pallas_call(
        functools.partial(stream, classes, subs, given),
        out_shape=(
            jax.ShapeDtypeStruct((rows, ncol, lane), f32),
            jax.ShapeDtypeStruct((classes - 1, lead, unit, lane), f32),
            jax.ShapeDtypeStruct((chunks, blocks, depth, width), f32),
        ),
        in_specs=[pl.BlockSpec(memory_space=pl.ANY)] * 2,
        out_specs=(pl.BlockSpec(memory_space=pl.ANY),) * 3,
        scratch_shapes=[
            pltpu.VMEM((rows, ncol, lane), f32),
            pltpu.VMEM((chunks, blocks, q, width), f32),
            pltpu.VMEM((2, lead, unit, lane), f32),
            pltpu.VMEM((bands, classes * rows, blocks * lane), bf16),
            pltpu.VMEM((bands, classes * rows, blocks * lane), bf16),
            pltpu.VMEM((2, blocks, lane, width), f32),
            pltpu.VMEM((blocks * lane, width), bf16),
            pltpu.VMEM((blocks * lane, width), bf16),
            pltpu.VMEM((min(SLOTS, chunks), per, classes, rows, lane), f32),
            pltpu.VMEM((chunks + given, per, classes - 1, rows, lane), f32),
            pltpu.VMEM((classes, rows, deep), f32),
            pltpu.VMEM((classes * rows, deep), bf16),
            pltpu.VMEM((classes * rows, deep), bf16),
            pltpu.VMEM((some, per, rows, lane), f32),
            dma((classes,)),
            dma((classes,)),
            dma((classes,)),
            dma((classes,)),
            dma((some,)),
            dma((some,)),
            dma((2, chunks)),
            dma((2, chunks, spots)),
            dma((2, chunks, spots)),
            dma((chunks, spots)),
            dma((chunks, spots)),
            dma((chunks,)),
            dma((chunks + given, per, levels)),
            dma((chunks + given, per, levels)),
            dma((2,)),
            dma((2,)),
            dma((ncol // sub,)),
        ],
        compiler_params=pltpu.CompilerParams(
            collective_id=0, has_side_effects=True, vmem_limit_bytes=62 * 1024 * 1024
        ),
    )(left, right)
    out = out.reshape(rows, halves, wide // lane, cols, lane)
    return jnp.transpose(out, (0, 1, 3, 2, 4)).reshape(b_blocks.shape)


def fits(classes, subs, first_factor_tiles, b_blocks):
    blocks, q, halves, cols, order = first_factor_tiles.shape
    bands, spots = order // (LANE * classes), subs // 2
    return (
        classes > 1 and bands > 1 and q % SUBLANE == 0 and order % (LANE * classes) == 0 and (bands * cols) % SUBLANE == 0
        and bands * LANE == subs * q and spots % bands == 0
    )


def either(classes, subs, first_factor_tiles, b_blocks):
    pick = streamed if fits(classes, subs, first_factor_tiles, b_blocks) else local
    return pick(classes, subs, first_factor_tiles, b_blocks)


def solution(mesh):
    spec = P(None, ("cls", "str"), None, None, None)
    return jax.shard_map(
        functools.partial(either, mesh.shape["cls"], mesh.shape["str"]),
        mesh=mesh, in_specs=(spec, spec), out_specs=spec, check_vma=False,
    )
```

```python
import functools

import jax
import jax.numpy as jnp
from jax import lax
from jax.experimental import pallas as pl
from jax.experimental.pallas import tpu as pltpu
from jax.sharding import PartitionSpec as P

MESH = pl.DeviceIdType.MESH
LAG = 3
EARLY = 2
AHEAD = 7
OUTER = 2
EARLY_RELAYS = ((3, 2), (5, 3), (7, 5))
TURN = 1
BLOCK = 2
LEAD = 2
MORE = 2
GIVEN = 2
SLOTS = 8
CALM = 15
LANE = 128
SUBLANE = 8


def flip(index, mask, count):
    out, bit = index, 1
    while bit < count:
        have, want = (index // bit) % 2, (mask // bit) % 2
        out = out + want * (1 - 2 * have) * bit
        bit *= 2
    return out


def kernel(
    classes, subs, a_ref, b_ref, o_ref, aland, ball,
    ahi, alo, astage, bstage, bhi, blo, cpart, rland,
    a_send, a_recv, own_send, fwd_send, line_recv, peer_send, peer_recv,
    c_send, c_recv, a_load, b_load, o_sem,
):
    chunks, groups, piece, width = b_ref.shape
    rows = a_ref.shape[1]
    depth = subs * piece
    spots = subs // 2
    c, s = lax.axis_index("cls"), lax.axis_index("str")
    spot, core = s // 2, s % 2
    mate = (c, s + 1 - 2 * core)
    beside = ((c, s - 2), (c, s + 2))
    has = (spot > 0, spot < spots - 1)

    barrier = pltpu.get_barrier_semaphore()
    for d in range(1, classes):
        pl.semaphore_signal(barrier, inc=1, device_id=(flip(c, d, classes), s), device_id_type=MESH)
    pl.semaphore_signal(barrier, inc=1, device_id=mate, device_id_type=MESH)
    for side in range(2):
        @pl.when(has[side])
        def _():
            pl.semaphore_signal(barrier, inc=1, device_id=beside[side], device_id_type=MESH)
    lower, higher = (spot + spots - 1) // spots, (2 * spots - 2 - spot) // spots
    pl.semaphore_wait(barrier, classes + lower + higher)

    def remote(src, dst, send, recv, to):
        return pltpu.make_async_remote_copy(
            src_ref=src, dst_ref=dst, send_sem=send, recv_sem=recv,
            device_id=to, device_id_type=MESH,
        )

    def slot(j, owner):
        return ball.at[j, :, pl.ds(pl.multiple_of(owner * piece, piece), piece), :]

    def own_line(j, side):
        return remote(b_ref.at[j], slot(j, s), own_send.at[side, j], line_recv.at[side, j, 0], beside[side])

    def own_mate(j):
        return remote(b_ref.at[j], slot(j, s), peer_send.at[j, spot], peer_recv.at[j, spot], mate)

    def origin(side, dist):
        return spot + dist if side == 0 else spot - dist

    def there(side, dist):
        return spot + dist < spots if side == 0 else spot >= dist

    def arrival(j, side, dist):
        at = slot(j, 2 * origin(side, dist) + core)
        return remote(at, at, own_send.at[side, j], line_recv.at[side, j, dist - 1], beside[1 - side])

    def onward(j, side, dist):
        at = slot(j, 2 * origin(side, dist) + core)
        return remote(at, at, fwd_send.at[side, j, dist - 1], line_recv.at[side, j, dist], beside[side])

    def across(j, side, dist):
        begin = origin(side, dist)
        at = slot(j, 2 * begin + core)
        return remote(at, at, peer_send.at[j, begin], peer_recv.at[j, begin], mate)

    def forward(j, dist):
        for side in range(2):
            @pl.when(there(side, dist))
            def _():
                arrival(j, side, dist).wait_recv()

                @pl.when(has[side])
                def _():
                    onward(j, side, dist).start()

                across(j, side, dist).start()

    def a_copy(d):
        peer = flip(c, d, classes)
        return remote(
            a_ref.at[:, :, pl.ds(pl.multiple_of(peer * depth, depth), depth)],
            aland.at[:, pl.ds(pl.multiple_of(c * rows, rows), rows), :],
            a_send.at[d], a_recv.at[d], (peer, s),
        )

    for d in range(1, classes):
        a_copy(d).start()

    def begin(j, _):
        for side in range(2):
            @pl.when(has[side])
            def _():
                own_line(j, side).start()
        own_mate(j).start()
        return 0

    lax.fori_loop(0, chunks, begin, 0)

    for j in range(min(EARLY, chunks)):
        forward(j, 1)
    for d in range(1, classes):
        a_copy(d).wait_recv()

    def load_a(g, held):
        for e in range(classes):
            to = astage.at[held, pl.ds(e * rows, rows), :]

            @pl.when(c == e)
            def _():
                pltpu.make_async_copy(
                    a_ref.at[g, :, pl.ds(pl.multiple_of(c * depth, depth), depth)], to, a_load.at[held]
                ).start()

            @pl.when(c != e)
            def _():
                pltpu.make_async_copy(aland.at[g, pl.ds(e * rows, rows), :], to, a_load.at[held]).start()

    load_a(0, 0)
    for g in range(groups):
        held = g % 2
        if g + 1 < groups:
            load_a(g + 1, 1 - held)
        pltpu.make_async_copy(aland.at[g], astage.at[held], a_load.at[held]).wait()

        def split(m, _, held=held, g=g):
            at = pl.ds(pl.multiple_of(m * rows, rows), rows)
            value = astage[held, at, :]
            high = value.astype(jnp.bfloat16)
            ahi[at, g * depth:(g + 1) * depth] = high
            alo[at, g * depth:(g + 1) * depth] = (value - high.astype(jnp.float32)).astype(jnp.bfloat16)
            return 0

        lax.fori_loop(0, classes, split, 0)

    def c_copy(j, d):
        peer = flip(c, d, classes)
        return remote(
            cpart.at[j, pl.ds(pl.multiple_of(peer * rows, rows), rows), :],
            rland.at[j, d - 1], c_send.at[j, d], c_recv.at[j, d], (peer, s),
        )

    mine = pl.ds(pl.multiple_of(c * rows, rows), rows)

    def out_copy(j):
        return pltpu.make_async_copy(cpart.at[j, mine, :], o_ref.at[j], o_sem.at[j])

    def reduce(j):
        for d in range(1, classes):
            c_copy(j, d).wait_recv()
        total = cpart[j, mine, :]
        for d in range(1, classes):
            total = total + rland[j, d - 1]
        cpart[j, mine, :] = total
        out_copy(j).start()

    def step(j, _):
        if spots > 1:
            @pl.when(j + EARLY < chunks)
            def _():
                forward(j + EARLY, 1)
        for dist in range(2, spots):
            forward(j, dist)

        for owner in range(subs):
            to = bstage.at[:, pl.ds(owner * piece, piece), :]

            @pl.when(s == owner)
            def _():
                pltpu.make_async_copy(b_ref.at[j], to, b_load.at[0]).start()

            @pl.when(s != owner)
            def _():
                @pl.when(core != owner % 2)
                def _():
                    remote(to_slot(j, owner), to_slot(j, owner), peer_send.at[j, owner // 2],
                           peer_recv.at[j, owner // 2], mate).wait_recv()

                pltpu.make_async_copy(to_slot(j, owner), to, b_load.at[0]).start()

        pltpu.make_async_copy(ball.at[j], bstage, b_load.at[0]).wait()

        def split(g, _):
            value = bstage[g]
            high = value.astype(jnp.bfloat16)
            at = pl.ds(pl.multiple_of(g * depth, depth), depth)
            bhi[at, :] = high
            blo[at, :] = (value - high.astype(jnp.float32)).astype(jnp.bfloat16)
            return 0

        lax.fori_loop(0, groups, split, 0)

        def part(i, _):
            d = (i + 1) % classes
            at = pl.ds(pl.multiple_of(flip(c, d, classes) * rows, rows), rows)
            dot = functools.partial(jnp.dot, preferred_element_type=jnp.float32)
            cpart[j, at, :] = (
                dot(ahi[at, :], bhi[...]) + dot(ahi[at, :], blo[...]) + dot(alo[at, :], bhi[...])
            )

            @pl.when(d != 0)
            def _():
                c_copy(j, d).start()

            return 0

        lax.fori_loop(0, classes, part, 0)

        @pl.when(j >= LAG)
        def _():
            reduce(j - LAG)

        return 0

    def to_slot(j, owner):
        return ball.at[j, :, pl.ds(owner * piece, piece), :]

    lax.fori_loop(0, chunks, step, 0)
    for j in range(max(chunks - LAG, 0), chunks):
        reduce(j)

    def finish(j, _):
        out_copy(j).wait()
        own_mate(j).wait_send()
        for d in range(1, classes):
            c_copy(j, d).wait_send()
        for side in range(2):
            @pl.when(has[side])
            def _():
                own_line(j, side).wait_send()
            for dist in range(1, spots):
                @pl.when(there(side, dist))
                def _():
                    @pl.when(has[side])
                    def _():
                        onward(j, side, dist).wait_send()
                    across(j, side, dist).wait_send()
        return 0

    lax.fori_loop(0, chunks, finish, 0)
    for d in range(1, classes):
        a_copy(d).wait_send()


def local(classes, subs, first_factor_tiles, b_blocks):
    blocks, q, halves, cols, order = first_factor_tiles.shape
    inner, width = halves * cols, b_blocks.shape[4]
    rows = blocks * q
    left = first_factor_tiles.reshape(rows, inner, order)
    right = jnp.transpose(b_blocks.reshape(inner, q, inner, width), (2, 0, 1, 3))
    if q % 8 == 0:
        left = jnp.transpose(left, (1, 0, 2))
    else:
        left = left.reshape(rows, inner, classes * subs, q)
        left = jnp.transpose(left, (0, 2, 1, 3)).reshape(1, rows, inner * order)
        right = right.reshape(inner, 1, inner * q, width)
    chunks, groups, piece, _ = right.shape
    depth = subs * piece
    dma = pltpu.SemaphoreType.DMA
    f32, bf16 = jnp.float32, jnp.bfloat16
    spots = subs // 2
    out, _, _ = pl.pallas_call(
        functools.partial(kernel, classes, subs),
        out_shape=(
            jax.ShapeDtypeStruct((chunks, rows, width), f32),
            jax.ShapeDtypeStruct((groups, classes * rows, depth), f32),
            jax.ShapeDtypeStruct((chunks, groups, depth, width), f32),
        ),
        in_specs=[pl.BlockSpec(memory_space=pl.ANY)] * 2,
        out_specs=(pl.BlockSpec(memory_space=pl.ANY),) * 3,
        scratch_shapes=[
            pltpu.VMEM((classes * rows, groups * depth), bf16),
            pltpu.VMEM((classes * rows, groups * depth), bf16),
            pltpu.VMEM((2, classes * rows, depth), f32),
            pltpu.VMEM((groups, depth, width), f32),
            pltpu.VMEM((groups * depth, width), bf16),
            pltpu.VMEM((groups * depth, width), bf16),
            pltpu.VMEM((chunks, classes * rows, width), f32),
            pltpu.VMEM((chunks, classes - 1, rows, width), f32),
            dma((classes,)),
            dma((classes,)),
            dma((2, chunks)),
            dma((2, chunks, spots)),
            dma((2, chunks, spots)),
            dma((chunks, spots)),
            dma((chunks, spots)),
            dma((chunks, classes)),
            dma((chunks, classes)),
            dma((2,)),
            dma((1,)),
            dma((chunks,)),
        ],
        compiler_params=pltpu.CompilerParams(
            collective_id=0, has_side_effects=True, vmem_limit_bytes=60 * 1024 * 1024
        ),
    )(left, right)
    out = jnp.transpose(out, (1, 0, 2))
    return out.reshape(b_blocks.shape)


def stream(
    classes, subs, given, a_ref, b_ref, o_ref, aland, ball,
    flat, bown, astage, ahi, alo, bstage, bhi, blo, cpart, rland, lent, hhi, hlo, back,
    a_send, a_recv, lend_send, lend_recv, back_send, back_recv, own_send, fwd_send, line_recv, peer_send, peer_recv, keep_sem,
    c_send, c_recv, a_load, b_load, o_sem,
):
    lead, _, unit, lane = a_ref.shape
    rows, ncol, _ = b_ref.shape
    chunks, blocks, depth, width = ball.shape
    bands = depth // lane
    piece = depth // subs
    per = width // lane
    levels = classes.bit_length() - 1
    spots = subs // 2
    c, s = lax.axis_index("cls"), lax.axis_index("str")
    spot, core = s // 2, s % 2
    mate = (c, s + 1 - 2 * core)
    beside = ((c, s - 2), (c, s + 2))
    has = (spot > 0, spot < spots - 1)
    inner = (spot > 0) & (spot < spots - 1)
    outer = (spot == 0) | (spot == spots - 1)
    near = spot // (spots // bands)
    slots = cpart.shape[0]
    helps = (spot == 1) | (spot == spots - 2)
    total = jnp.where(helps, chunks + given, chunks)
    ends = (spot == 1, spot == spots - 2)
    friend = (c, jnp.where((spot == 0) | (spot == spots - 2), s + 2, s - 2))

    barrier = pltpu.get_barrier_semaphore()
    for d in range(1, classes):
        pl.semaphore_signal(barrier, inc=1, device_id=(flip(c, d, classes), s), device_id_type=MESH)
    pl.semaphore_signal(barrier, inc=1, device_id=mate, device_id_type=MESH)
    for side in range(2):
        @pl.when(has[side])
        def _():
            pl.semaphore_signal(barrier, inc=1, device_id=beside[side], device_id_type=MESH)
    share = ncol // o_sem.shape[0]

    def b_in(g):
        at = pl.ds(g * share, share)
        return pltpu.make_async_copy(b_ref.at[:, at, :], flat.at[:, at, :], o_sem.at[g])

    for g in range(o_sem.shape[0]):
        b_in(g).start()
    lower, higher = (spot + spots - 1) // spots, (2 * spots - 2 - spot) // spots
    pl.semaphore_wait(barrier, classes + lower + higher)

    def remote(src, dst, send, recv, to):
        return pltpu.make_async_remote_copy(
            src_ref=src, dst_ref=dst, send_sem=send, recv_sem=recv,
            device_id=to, device_id_type=MESH,
        )

    def a_copy(d):
        peer = flip(c, d, classes)
        return remote(a_ref.at[:, peer], aland.at[d - 1], a_send.at[d], a_recv.at[d], (peer, s))

    for d in range(1, classes):
        a_copy(d).start()

    def slot(j, owner):
        return ball.at[j, :, pl.ds(pl.multiple_of(owner * piece, piece), piece), :]

    def own_line(j, side):
        return remote(bown.at[j], slot(j, s), own_send.at[side, j], line_recv.at[side, j, 0], beside[side])

    def own_mate(j):
        return remote(bown.at[j], slot(j, s), peer_send.at[j, spot], peer_recv.at[j, spot], mate)

    def own_keep(j):
        return pltpu.make_async_copy(bown.at[j], slot(j, s), keep_sem.at[j])

    def origin(side, dist):
        return spot + dist if side == 0 else spot - dist

    def there(side, dist):
        return spot + dist < spots if side == 0 else spot >= dist

    def arrival(j, side, dist):
        at = slot(j, 2 * origin(side, dist) + core)
        return remote(at, at, own_send.at[side, j], line_recv.at[side, j, dist - 1], beside[1 - side])

    def onward(j, side, dist):
        at = slot(j, 2 * origin(side, dist) + core)
        return remote(at, at, fwd_send.at[side, j, dist - 1], line_recv.at[side, j, dist], beside[side])

    def across(j, side, dist):
        begin = origin(side, dist)
        at = slot(j, 2 * begin + core)
        return remote(at, at, peer_send.at[j, begin], peer_recv.at[j, begin], mate)

    def forward(j, dist):
        for side in range(2):
            @pl.when(gets(j, side, dist))
            def _():
                arrival(j, side, dist).wait_recv()

                @pl.when(feeds(j, side))
                def _():
                    onward(j, side, dist).start()

                across(j, side, dist).start()

    def relay(t, _):
        for dist in reversed(range(1, spots)):
            at = t - dist + 1 if dist > 1 else t

            @pl.when((at >= 0) & (at < chunks) & (inner | (dist == 1)))
            def _():
                forward(at, dist)

        @pl.when(inner & (t + LEAD < chunks))
        def _():
            own_out(t + LEAD)

        return 0

    def relay_far(t, _):
        @pl.when(outer & (t < chunks))
        def _():
            for dist in range(2, spots):
                forward(t, dist)

        return 0

    def relay_all(t, _):
        relay(t, 0)
        return relay_far(t, 0)

    def ready(t):
        slow = jnp.maximum(t + 1, given + OUTER + (t + 1) // 2)
        fast = AHEAD + 1 + (3 * t) // 4
        return jnp.minimum(jnp.where(inner, jnp.maximum(fast, t + spots), slow), chunks + spots - 2)

    def feeds(j, side):
        return has[side] & ((j >= given) | jnp.logical_not(ends[side]))

    def gets(j, side, dist):
        return there(side, dist) & ((j >= given) | inner)

    shift = given + MORE

    def own_out(j):
        for side in range(2):
            @pl.when(has[side] & jnp.logical_not(ends[side]))
            def _():
                own_line(j, side).start()

            @pl.when(ends[side] & (j + shift < chunks))
            def _():
                own_line(j + shift, side).start()

    rows_of = flat.reshape(rows * ncol, lane)

    def lay(j):
        for p in range(per):
            value = rows_of[pl.ds(j * per + p, rows, stride=ncol), :]
            bown[j, :, :, p * lane:(p + 1) * lane] = value.reshape(blocks, piece, lane)

    first = min(LEAD + shift, chunks)
    opened = 0
    for j in range(first):
        if j * per // share == opened:
            b_in(opened).wait()
            opened += 1
        lay(j)
        for side in range(2):
            if j < LEAD:
                @pl.when(has[side] & jnp.logical_not(ends[side]))
                def _():
                    own_line(j, side).start()

            if j >= given:
                @pl.when(ends[side])
                def _():
                    own_line(j, side).start()

    for g in range(opened, o_sem.shape[0]):
        b_in(g).wait()

    def lay_more(j, _):
        lay(j)
        return 0

    lax.fori_loop(first, chunks, lay_more, 0)

    def begin(j, _):
        own_mate(j).start()
        own_keep(j).start()

        @pl.when(outer & (j >= LEAD))
        def _():
            own_out(j)

        return 0

    lax.fori_loop(0, chunks, begin, 0)

    def take_a(d):
        held = astage.at[d % 2]
        if d == 0:
            return pltpu.make_async_copy(a_ref.at[:, c], held, a_load.at[0])
        return pltpu.make_async_copy(aland.at[d - 1], held, a_load.at[d % 2])

    def split_a(d):
        lines = astage.at[d % 2].reshape(lead * unit, lane)
        stride = lead * unit // rows
        cols = unit // bands

        def one(k, _):
            h, band, col = k // unit, (k % unit) // cols, k % cols
            value = lines[pl.ds(k, rows, stride=stride), :]
            high = value.astype(jnp.bfloat16)
            at = pl.ds(pl.multiple_of((h * cols + col) * lane, lane), lane)
            ahi[band, d * rows:(d + 1) * rows, at] = high
            alo[band, d * rows:(d + 1) * rows, at] = (value - high.astype(jnp.float32)).astype(jnp.bfloat16)
            return 0

        lax.fori_loop(0, stride, one, 0)

    def lend_copy(d):
        return remote(lent.at[d], lent.at[d], lend_send.at[d], lend_recv.at[d], friend)

    def lend(d):
        if not given:
            return
        lines = astage.at[d % 2].reshape(lead * unit, lane)
        stride = lead * unit // rows
        cols = unit // bands
        left = lax.broadcasted_iota(jnp.int32, (rows, lane), 1) < lane // 2
        low = spot % 2 == 1

        def block(g, band):
            return lines[pl.ds((g // cols) * unit + band * cols + g % cols, rows, stride=stride), :]

        @pl.when(outer)
        def _():
            for k in range(1, bands):
                def whole(g, _, k=k):
                    at = pl.ds(pl.multiple_of(((k - 1) * blocks + g) * lane, lane), lane)
                    lent[d, :, at] = block(g, (near + k) % bands)
                    return 0

                lax.fori_loop(0, blocks, whole, 0)

            def pair(g, _):
                one, two = block(2 * g, near), block(2 * g + 1, near)
                at = pl.ds(pl.multiple_of(((bands - 1) * blocks + g) * lane, lane), lane)
                lent[d, :, at] = jnp.where(
                    left,
                    jnp.where(low, one, pltpu.roll(one, lane // 2, 1)),
                    jnp.where(low, pltpu.roll(two, lane // 2, 1), two),
                )
                return 0

            lax.fori_loop(0, blocks // 2, pair, 0)
            lend_copy(d).start()

    take_a(0).start()
    take_a(0).wait()
    split_a(0)
    lend(0)

    def accept(d):
        a_copy(d).wait_recv()
        take_a(d).start()
        take_a(d).wait()
        split_a(d)
        lend(d)

    at = [jnp.where(inner, x, y) for x, y in EARLY_RELAYS]
    stops = [0] + [jnp.minimum(x, ready(-1)) for x in at]
    for d in range(1, classes):
        if d <= len(at):
            lax.fori_loop(stops[d - 1], stops[d], relay_all, 0)
        accept(d)
    lax.fori_loop(stops[min(len(at), classes - 1)], ready(-1), relay_all, 0)

    def order(p):
        return [(p + i) % levels for i in range(levels)]

    def place(p, d):
        at = 0
        for bit in order(p):
            at = 2 * at + (d // (1 << bit)) % 2
        return at

    def c_copy(j, p, level):
        count = classes >> (level + 1)
        peer = flip(c, 1 << order(p)[level], classes)
        return remote(
            cpart.at[j % slots, p, pl.ds(count, count)],
            rland.at[j, p, pl.ds(classes - 2 * count, count)],
            c_send.at[j, p, level], c_recv.at[j, p, level], (peer, s),
        )

    def out_copy(g):
        at = pl.ds(pl.multiple_of(g * share, share), share)
        return pltpu.make_async_copy(flat.at[:, at, :], o_ref.at[:, at, :], o_sem.at[g])

    turn = jnp.where(helps, chunks - TURN, chunks)

    def chunk_of(t):
        return jnp.where(helps & (t >= turn + given), t - given, t)

    def lent_at(t):
        return helps & (t >= turn) & (t < turn + given)

    late = -(-given * per // share)

    def back_copy(i):
        return remote(back.at[i], back.at[i], back_send.at[i], back_recv.at[i], friend)

    def reduce(j, level):
        count = classes >> (level + 1)
        held = j % slots
        for p in range(per):
            c_copy(j, p, level).wait_recv()
            if level + 1 < levels:
                cpart[held, p, 0:count] = (
                    cpart[held, p, 0:count] + rland[j, p, classes - 2 * count:classes - count]
                )
                c_copy(j, p, level + 1).start()
                continue

            @pl.when(jnp.logical_not(lent_at(j)))
            def _():
                rows_of[pl.ds(chunk_of(j) * per + p, rows, stride=ncol), :] = (
                    cpart[held, p, 0] + rland[j, p, classes - 2]
                )

            if given:
                @pl.when(lent_at(j))
                def _():
                    back[j - turn, p] = cpart[held, p, 0] + rland[j, p, classes - 2]
        if level + 1 == levels:
            count, done = share // per, chunk_of(j) + 1
            group = done // count - 1

            @pl.when(jnp.logical_not(lent_at(j)) & (done % count == 0) & (inner | (group >= late)))
            def _():
                out_copy(group).start()

            if given:
                @pl.when(lent_at(j))
                def _():
                    back_copy(j - turn).start()

    def gather(j, band):
        for owner in range(subs):
            @pl.when(owner // (subs // bands) == band)
            def _():
                @pl.when(s == owner)
                def _():
                    own_keep(j).wait()

                @pl.when((core != owner % 2) & (inner | (j >= given) | (spot == owner // 2)))
                def _():
                    at = slot(j, owner)
                    remote(at, at, peer_send.at[j, owner // 2], peer_recv.at[j, owner // 2], mate).wait_recv()

    def take_b(j, band, held):
        at = pl.ds(pl.multiple_of(band * lane, lane), lane)
        return pltpu.make_async_copy(ball.at[j, :, at, :], bstage.at[held], b_load.at[held])

    def split_b(held, size=lane, begin=0, step=lane):
        def split(g, _):
            value = bstage[held, g, 0:size, :]
            high = value.astype(jnp.bfloat16)
            at = pl.ds(pl.multiple_of(g * step + begin, size), size)
            bhi[at, :] = high
            blo[at, :] = (value - high.astype(jnp.float32)).astype(jnp.bfloat16)
            return 0

        lax.fori_loop(0, blocks, split, 0)

    part_rows = 2 * piece

    def take_part(j, held):
        at = pl.ds(pl.multiple_of(spot * part_rows, part_rows), part_rows)
        return pltpu.make_async_copy(
            ball.at[j, :, at, :], bstage.at[held, :, pl.ds(0, part_rows), :], b_load.at[held]
        )

    def clear_part(begin):
        def clear(g, _):
            at = pl.ds(pl.multiple_of(g * lane + begin, part_rows), part_rows)
            bhi[at, :] = jnp.zeros((part_rows, width), jnp.bfloat16)
            blo[at, :] = jnp.zeros((part_rows, width), jnp.bfloat16)
            return 0

        lax.fori_loop(0, blocks, clear, 0)

    def settle(j):
        for p in range(per):
            for level in range(levels):
                c_copy(j, p, level).wait_send()

    def multiply(j, left, deep, first):
        dot = functools.partial(jnp.dot, preferred_element_type=jnp.float32)
        held = j % slots

        def part(i, _):
            at = pl.ds(pl.multiple_of(i * BLOCK * rows, rows), BLOCK * rows)
            high, low = left(at)
            total = dot(high, bhi[0:deep]) + dot(high, blo[0:deep]) + dot(low, bhi[0:deep])
            for p in range(per):
                for k in range(BLOCK):
                    value = total[k * rows:(k + 1) * rows, p * lane:(p + 1) * lane]
                    to = place(p, i * BLOCK + k)
                    cpart[held, p, to] = value if first else cpart[held, p, to] + value
            return 0

        lax.fori_loop(0, classes // BLOCK, part, 0)

    def mine(band):
        return lambda at: (ahi[band, at, :], alo[band, at, :])

    def theirs(begin, deep):
        return lambda at: (hhi[at, begin:begin + deep], hlo[at, begin:begin + deep])

    def sum_first(k, _):
        reduce(k, 0)
        return 0

    def sum_rest(k, _):
        for level in range(1, levels):
            reduce(k, level)
        return 0

    calm = jnp.where(outer, chunks * CALM // 16, chunks + given)

    def first_sums(j):
        return jnp.where(j > calm, j, jnp.maximum(j - 1, 0))

    def last_sums(j):
        return jnp.where(j > calm, j, jnp.maximum(j - 2, 0))

    def sums(body, begin, end):
        lax.fori_loop(begin, jnp.maximum(begin, end), body, 0)

    def usual(t):
        j = chunk_of(t)
        lax.fori_loop(ready(j - 1), ready(j), relay, 0)
        alone = outer & (j < given)
        whole = inner | (j >= given)
        gather(j, near)

        @pl.when(whole)
        def _():
            take_b(j, near, 0).start()

        @pl.when(inner)
        def _():
            gather(j, (near + 1) % bands)
            take_b(j, (near + 1) % bands, 1).start()

        if given:
            @pl.when(alone)
            def _():
                take_part(j, 0).start()

        sums(sum_first, first_sums(t - 1), t - 1)

        @pl.when(t >= slots)
        def _():
            settle(t - slots)

        @pl.when(whole)
        def _():
            take_b(j, near, 0).wait()
            split_b(0)

        if given:
            @pl.when(alone)
            def _():
                take_part(j, 0).wait()
                split_b(0, part_rows, (spot % 2) * part_rows)
                clear_part((1 - spot % 2) * part_rows)

        multiply(t, mine(near), blocks * lane, True)
        sums(sum_first, jnp.maximum(t - 1, 0), first_sums(t))
        lax.fori_loop(ready(j - 1), ready(j), relay_far, 0)

        @pl.when(whole)
        def _():
            for k in range(1, bands):
                band = (near + k) % bands

                @pl.when(outer | (k > 1))
                def _():
                    gather(j, band)
                    take_b(j, band, k % 2).start()

                if k == 1:
                    sums(sum_rest, last_sums(t - 1), t - 2)
                take_b(j, band, k % 2).wait()
                split_b(k % 2)
                multiply(t, mine(band), blocks * lane, False)

        @pl.when(alone)
        def _():
            sums(sum_rest, last_sums(t - 1), t - 2)

    def take_lent(d):
        lend_copy(d).wait_recv()

        def one(g, _):
            at = pl.ds(pl.multiple_of(g * lane, lane), lane)
            value = lent[d, :, at]
            high = value.astype(jnp.bfloat16)
            hhi[d * rows:(d + 1) * rows, at] = high
            hlo[d * rows:(d + 1) * rows, at] = (value - high.astype(jnp.float32)).astype(jnp.bfloat16)
            return 0

        lax.fori_loop(0, lent.shape[2] // lane, one, 0)

    def extra(t):
        i = t - turn
        take_part(i, 0).start()
        for k in range(1, bands):
            if k == 1:
                take_b(i, (near + k) % bands, k % 2).start()
        sums(sum_first, first_sums(t - 1), first_sums(t))

        @pl.when(t >= slots)
        def _():
            settle(t - slots)

        @pl.when(i == 0)
        def _():
            for d in range(classes):
                take_lent(d)

        take_part(i, 0).wait()
        split_b(0, part_rows, 0, part_rows)
        multiply(t, theirs((bands - 1) * blocks * lane, blocks * part_rows), blocks * part_rows, True)
        for k in range(1, bands):
            if k > 1:
                take_b(i, (near + k) % bands, k % 2).start()
            if k == 1:
                sums(sum_rest, last_sums(t - 1), last_sums(t))
            take_b(i, (near + k) % bands, k % 2).wait()
            split_b(k % 2)
            multiply(t, theirs((k - 1) * blocks * lane, blocks * lane), blocks * lane, False)

    def step(t, _):
        if given:
            @pl.when(lent_at(t))
            def _():
                extra(t)

        @pl.when(jnp.logical_not(lent_at(t)))
        def _():
            usual(t)

        for p in range(per):
            c_copy(t, p, 0).start()
        sums(sum_rest, jnp.maximum(last_sums(t - 1), t - 2), last_sums(t))
        return 0

    lax.fori_loop(0, total, step, 0)

    def last(k, _):
        reduce(k, 0)

        @pl.when(k > last_sums(total - 1))
        def _():
            sum_rest(k - 1, 0)

        return 0

    lax.fori_loop(first_sums(total - 1), total, last, 0)
    sum_rest(total - 1, 0)

    if given:
        @pl.when(outer)
        def _():
            for i in range(given):
                back_copy(i).wait_recv()
                for p in range(per):
                    at = pl.ds(i * per + p, rows, stride=ncol)
                    rows_of[at, :] = rows_of[at, :] + back[i, p]
            for g in range(late):
                out_copy(g).start()

    for g in range(o_sem.shape[0]):
        out_copy(g).wait()

    def finish(j, _):
        own_mate(j).wait_send()
        for side in range(2):
            @pl.when(feeds(j, side))
            def _():
                own_line(j, side).wait_send()
            for dist in range(1, spots):
                @pl.when(gets(j, side, dist))
                def _():
                    @pl.when(feeds(j, side))
                    def _():
                        onward(j, side, dist).wait_send()
                    across(j, side, dist).wait_send()
        return 0

    lax.fori_loop(0, chunks, finish, 0)

    def settled(j, _):
        settle(j)
        return 0

    lax.fori_loop(total - slots, total, settled, 0)
    for d in range(1, classes):
        a_copy(d).wait_send()
    if given:
        @pl.when(outer)
        def _():
            for d in range(classes):
                lend_copy(d).wait_send()

        @pl.when(helps)
        def _():
            for i in range(given):
                back_copy(i).wait_send()


def streamed(classes, subs, first_factor_tiles, b_blocks):
    blocks, q, halves, cols, order = first_factor_tiles.shape
    wide = b_blocks.shape[4]
    lane, sub = LANE, SUBLANE
    rows, bands, ncol = blocks * q, order // (LANE * classes), halves * cols * wide // LANE
    left = first_factor_tiles.reshape(rows, halves, cols, classes * bands, lane)
    left = jnp.transpose(left, (0, 1, 3, 2, 4)).reshape(rows * halves, classes, bands * cols, lane)
    right = b_blocks.reshape(rows, halves, cols, wide // lane, lane)
    right = jnp.transpose(right, (0, 1, 3, 2, 4)).reshape(rows, ncol, lane)
    lead, unit = rows * halves, bands * cols
    per = 2
    chunks, width, depth = ncol // per, per * lane, bands * lane
    dma = pltpu.SemaphoreType.DMA
    f32, bf16 = jnp.float32, jnp.bfloat16
    spots, levels = subs // 2, classes.bit_length() - 1
    given = chunks * GIVEN // 16 if spots > 3 and spots == 2 * bands and blocks % 2 == 0 else 0
    deep = (2 * bands - 1) * blocks * lane // 2
    some = max(given, 1)
    out, _, _ = pl.pallas_call(
        functools.partial(stream, classes, subs, given),
        out_shape=(
            jax.ShapeDtypeStruct((rows, ncol, lane), f32),
            jax.ShapeDtypeStruct((classes - 1, lead, unit, lane), f32),
            jax.ShapeDtypeStruct((chunks, blocks, depth, width), f32),
        ),
        in_specs=[pl.BlockSpec(memory_space=pl.ANY)] * 2,
        out_specs=(pl.BlockSpec(memory_space=pl.ANY),) * 3,
        scratch_shapes=[
            pltpu.VMEM((rows, ncol, lane), f32),
            pltpu.VMEM((chunks, blocks, q, width), f32),
            pltpu.VMEM((2, lead, unit, lane), f32),
            pltpu.VMEM((bands, classes * rows, blocks * lane), bf16),
            pltpu.VMEM((bands, classes * rows, blocks * lane), bf16),
            pltpu.VMEM((2, blocks, lane, width), f32),
            pltpu.VMEM((blocks * lane, width), bf16),
            pltpu.VMEM((blocks * lane, width), bf16),
            pltpu.VMEM((min(SLOTS, chunks), per, classes, rows, lane), f32),
            pltpu.VMEM((chunks + given, per, classes - 1, rows, lane), f32),
            pltpu.VMEM((classes, rows, deep), f32),
            pltpu.VMEM((classes * rows, deep), bf16),
            pltpu.VMEM((classes * rows, deep), bf16),
            pltpu.VMEM((some, per, rows, lane), f32),
            dma((classes,)),
            dma((classes,)),
            dma((classes,)),
            dma((classes,)),
            dma((some,)),
            dma((some,)),
            dma((2, chunks)),
            dma((2, chunks, spots)),
            dma((2, chunks, spots)),
            dma((chunks, spots)),
            dma((chunks, spots)),
            dma((chunks,)),
            dma((chunks + given, per, levels)),
            dma((chunks + given, per, levels)),
            dma((2,)),
            dma((2,)),
            dma((ncol // sub,)),
        ],
        compiler_params=pltpu.CompilerParams(
            collective_id=0, has_side_effects=True, vmem_limit_bytes=62 * 1024 * 1024
        ),
    )(left, right)
    out = out.reshape(rows, halves, wide // lane, cols, lane)
    return jnp.transpose(out, (0, 1, 3, 2, 4)).reshape(b_blocks.shape)


def fits(classes, subs, first_factor_tiles, b_blocks):
    blocks, q, halves, cols, order = first_factor_tiles.shape
    bands, spots = order // (LANE * classes), subs // 2
    return (
        classes > 1 and bands > 1 and q % SUBLANE == 0 and order % (LANE * classes) == 0 and (bands * cols) % SUBLANE == 0
        and bands * LANE == subs * q and spots % bands == 0
    )


def either(classes, subs, first_factor_tiles, b_blocks):
    pick = streamed if fits(classes, subs, first_factor_tiles, b_blocks) else local
    return pick(classes, subs, first_factor_tiles, b_blocks)


def solution(mesh):
    spec = P(None, ("cls", "str"), None, None, None)
    return jax.shard_map(
        functools.partial(either, mesh.shape["cls"], mesh.shape["str"]),
        mesh=mesh, in_specs=(spec, spec), out_specs=spec, check_vma=False,
    )
```
